16 devices in a mesh: dp: 2 (over y, z), cp: 8 (over x, core).
Axes of the slice: x: 4, y: 2, z: 1, core: 2. Of those that a mesh axis runs over, the one named last changes fastest.
The devices are a block of a 4x4x8 slice.
Arguments:
- x_in: bfloat16 [4096, 1536], P(('dp', 'cp')), parts along dimension 0
- d_y: bfloat16 [4096, 1536], P(('dp', 'cp')), parts along dimension 0
- w_q: bfloat16 [1536, 12, 128], replicated
- w_k: bfloat16 [1536, 2, 128], replicated
- w_v: bfloat16 [1536, 2, 128], replicated
- w_o: bfloat16 [12, 128, 1536], replicated
Outputs:
- output: bfloat16 [4096, 1536], P(('dp', 'cp')), parts along dimension 0
There are 2 independent parts. The reference program is written for one: setup_inputs(seed, part) draws one part's arguments, and reference() takes and returns one part's arrays. A program takes and returns all parts, laid end to end along the dimension named above; an argument that names none is the same for every part.
All inputs are finite; a program needn't handle non-finite values.
Results may differ from the reference program's by a relative error of at most 0.0113783.
Values are sent between devices in bfloat16 or wider.
A program may use at most 768 MiB of HBM per device.

```python
import jax
import jax.numpy as jnp
from jax import lax

D_MODEL = 1536
Q_HEADS = 12
KV_HEADS = 2
HEAD_DIM = 128
TOK_DEV = 256
CP_SIZE = 8
ROW_BLOCK = 32
SEQ_LEN = CP_SIZE * TOK_DEV
SEG_LEN = TOK_DEV // 2
Q_GROUP = Q_HEADS // KV_HEADS
SCORE_SCALE = HEAD_DIM ** -0.5
DY_SCALE = (SEQ_LEN / 16) ** 0.5


def token_positions(row_ids):
    dev_idx = row_ids // TOK_DEV
    row_off = row_ids % TOK_DEV
    seg_idx = jnp.where(row_off < SEG_LEN, dev_idx, 2 * CP_SIZE - 1 - dev_idx)
    return seg_idx * SEG_LEN + row_off % SEG_LEN


def setup_inputs(seed: int = 0, part: int = 0) -> dict:
    part_key = jax.random.fold_in(jax.random.key(seed), part)
    key_x, key_dy = jax.random.split(part_key)
    key_q, key_k, key_v, key_o = jax.random.split(jax.random.key(seed + 1), 4)
    x_in = jax.random.normal(key_x, (SEQ_LEN, D_MODEL), jnp.float32).astype(jnp.bfloat16)
    d_y = (jax.random.normal(key_dy, (SEQ_LEN, D_MODEL), jnp.float32) * DY_SCALE).astype(jnp.bfloat16)
    w_q = (jax.random.normal(key_q, (D_MODEL, Q_HEADS, HEAD_DIM), jnp.float32) * D_MODEL ** -0.5).astype(jnp.bfloat16)
    w_k = (jax.random.normal(key_k, (D_MODEL, KV_HEADS, HEAD_DIM), jnp.float32) * D_MODEL ** -0.5).astype(jnp.bfloat16)
    w_v = (jax.random.normal(key_v, (D_MODEL, KV_HEADS, HEAD_DIM), jnp.float32) * D_MODEL ** -0.5).astype(jnp.bfloat16)
    w_o = (jax.random.normal(key_o, (Q_HEADS, HEAD_DIM, D_MODEL), jnp.float32) * (Q_HEADS * HEAD_DIM) ** -0.5).astype(jnp.bfloat16)
    return {"x_in": x_in, "d_y": d_y, "w_q": w_q, "w_k": w_k, "w_v": w_v, "w_o": w_o}


def reference(x_in, d_y, w_q, w_k, w_v, w_o):
    wq_flat = w_q.reshape(D_MODEL, Q_HEADS * HEAD_DIM)
    wk_flat = w_k.reshape(D_MODEL, KV_HEADS * HEAD_DIM)
    wv_flat = w_v.reshape(D_MODEL, KV_HEADS * HEAD_DIM)
    wo_flat = w_o.reshape(Q_HEADS * HEAD_DIM, D_MODEL)
    q_proj = jnp.dot(x_in, wq_flat, preferred_element_type=jnp.float32).astype(jnp.bfloat16)
    k_proj = jnp.dot(x_in, wk_flat, preferred_element_type=jnp.float32).astype(jnp.bfloat16)
    v_proj = jnp.dot(x_in, wv_flat, preferred_element_type=jnp.float32).astype(jnp.bfloat16)
    do_proj = jnp.dot(d_y, wo_flat.T, preferred_element_type=jnp.float32).astype(jnp.bfloat16)
    queries = q_proj.astype(jnp.float32).reshape(SEQ_LEN, KV_HEADS, Q_GROUP, HEAD_DIM)
    key_all = k_proj.astype(jnp.float32).reshape(SEQ_LEN, KV_HEADS, HEAD_DIM)
    val_all = v_proj.astype(jnp.float32).reshape(SEQ_LEN, KV_HEADS, HEAD_DIM)
    d_out = do_proj.astype(jnp.float32).reshape(SEQ_LEN, KV_HEADS, Q_GROUP, HEAD_DIM)
    positions = token_positions(jnp.arange(SEQ_LEN))

    def block_step(acc_pair, blk_idx):
        dk_acc, dv_acc = acc_pair
        row_start = blk_idx * ROW_BLOCK
        q_blk = lax.dynamic_slice_in_dim(queries, row_start, ROW_BLOCK, 0)
        do_blk = lax.dynamic_slice_in_dim(d_out, row_start, ROW_BLOCK, 0)
        pos_blk = lax.dynamic_slice_in_dim(positions, row_start, ROW_BLOCK, 0)
        scores = jnp.einsum("rkge,ske->krgs", q_blk, key_all) * SCORE_SCALE
        causal = pos_blk[None, :, None, None] >= positions[None, None, None, :]
        scores = jnp.where(causal, scores, -jnp.inf)
        lse_blk = jax.nn.logsumexp(scores, axis=-1, keepdims=True)
        prob_blk = jnp.exp(scores - lse_blk).astype(jnp.bfloat16).astype(jnp.float32)
        out_blk = jnp.einsum("krgs,ske->krge", prob_blk, val_all).astype(jnp.bfloat16).astype(jnp.float32)
        row_delta = jnp.einsum("rkge,krge->krg", do_blk, out_blk)
        dp_blk = jnp.einsum("rkge,ske->krgs", do_blk, val_all)
        ds_blk = (prob_blk * (dp_blk - row_delta[..., None])).astype(jnp.bfloat16).astype(jnp.float32)
        dq_blk = (jnp.einsum("krgs,ske->rkge", ds_blk, key_all) * SCORE_SCALE).astype(jnp.bfloat16)
        dk_acc = dk_acc + jnp.einsum("krgs,rkge->ske", ds_blk, q_blk)
        dv_acc = dv_acc + jnp.einsum("krgs,rkge->ske", prob_blk, do_blk)
        return (dk_acc, dv_acc), dq_blk

    zero_acc = jnp.zeros((SEQ_LEN, KV_HEADS, HEAD_DIM), jnp.float32)
    (dk_sum, dv_sum), dq_blocks = lax.scan(block_step, (zero_acc, zero_acc), jnp.arange(SEQ_LEN // ROW_BLOCK))
    d_query = dq_blocks.reshape(SEQ_LEN, Q_HEADS * HEAD_DIM)
    d_key = (dk_sum * SCORE_SCALE).astype(jnp.bfloat16).reshape(SEQ_LEN, KV_HEADS * HEAD_DIM)
    d_value = dv_sum.astype(jnp.bfloat16).reshape(SEQ_LEN, KV_HEADS * HEAD_DIM)
    d_x = jnp.dot(d_query, wq_flat.T, preferred_element_type=jnp.float32)
    d_x = d_x + jnp.dot(d_key, wk_flat.T, preferred_element_type=jnp.float32)
    d_x = d_x + jnp.dot(d_value, wv_flat.T, preferred_element_type=jnp.float32)
    return d_x.astype(jnp.bfloat16)
```

```python
import functools
import math

import jax
import jax.numpy as jnp
from jax import lax
from jax.experimental import pallas as pl
from jax.experimental.pallas import tpu as pltpu
from jax.sharding import PartitionSpec as P

MESH = pl.DeviceIdType.MESH
BF = jnp.bfloat16
F32 = jnp.float32
OWN, LF, RT, OP = 0, 1, 2, 3
NT = (((1,), (1,)), ((), ()))


def dot(a, b):
    return jnp.dot(a, b, preferred_element_type=F32)


def dot_nt(a, b):
    return lax.dot_general(a, b, NT, preferred_element_type=F32)


def kernel(n_dev, x_hbm, dy_hbm, wq_hbm, wk_hbm, wv_hbm, wo_hbm, out_hbm,
           x_v, dy_v, wq_v, wk_v, wv_v, wo_v, wf_v, wkv_v,
           kv_send, kvbuf, q_send, do_send, qbuf, dobuf,
           est, dpst, m_run, l_run, d_run, m_ent, p_buf, ds_buf, dqt,
           pacc, pown, m1_lf, m1_rt, fin, fin_own, dq_send, dq_rows, acc, out_v, dkv, dq_tmp,
           ld_sem, st_sem, kvs, kvr, kvps, kvrs, qs, qr, m1s, m1r, m2s, m2r, fos, dqs, dqr):
    me = lax.axis_index("cp")
    n_chip = n_dev // 2
    c = me // 2
    h = me % 2
    ho = 1 - h
    right = lax.rem(c + 1, n_chip)
    left = lax.rem(c + n_chip - 1, n_chip)
    opp = lax.rem(c + 2, n_chip)
    rows, d_model = x_v.shape
    seg = rows // 2
    blk_len = kvbuf.shape[2]
    hd = qbuf.shape[3]
    groups = qbuf.shape[1]
    scale = hd ** -0.5
    scale2 = scale * math.log2(math.e)

    def off(blk, core):
        r = core if blk == 0 else 1 - core
        return pl.multiple_of(r * seg, seg)

    def rc(src, dst, ssem, rsem, chip, core):
        return pltpu.make_async_remote_copy(src_ref=src, dst_ref=dst, send_sem=ssem, recv_sem=rsem,
                                            device_id={"cp": chip * 2 + core}, device_id_type=MESH)

    loads = [pltpu.make_async_copy(a, b, ld_sem.at[i]) for i, (a, b) in enumerate([
        (wk_hbm, wk_v), (wv_hbm, wv_v), (x_hbm, x_v), (wq_hbm, wq_v), (dy_hbm, dy_v), (wo_hbm, wo_v)])]
    for cp in loads:
        cp.start()

    barrier = pltpu.get_barrier_semaphore()
    for chip, core in ((c, ho), (right, 0), (right, 1), (left, 0), (left, 1)):
        pl.semaphore_signal(barrier, inc=1, device_id={"cp": chip * 2 + core}, device_id_type=MESH)

    for j, (ld, w) in enumerate(((loads[0], wk_v), (loads[1], wv_v))):
        ld.wait()
        wf_v[...] = w[...].astype(F32)
        for hh in range(2):
            wkv_v[hh, :, j * hd:(j + 1) * hd] = wf_v[pl.ds(hh, d_model, stride=2), :].astype(BF)
    loads[2].wait()
    for hh in range(2):
        kv_send[hh] = dot(x_v[...], wkv_v[hh]).astype(BF)
    for blk in range(2):
        kvbuf[OWN, blk, pl.ds(off(blk, h), seg), :] = kv_send[h, blk * seg:(blk + 1) * seg, :]

    pl.semaphore_wait(barrier, 5)

    kv_sends = []
    for blk in range(2):
        kv_sends.append(rc(kv_send.at[ho, pl.ds(blk * seg, seg), :],
                           kvbuf.at[OWN, blk, pl.ds(off(blk, h), seg), :],
                           kvps.at[blk], kvr.at[OWN, h, blk], c, ho))
    dirs = []
    for first in range(2):
        go_right = (h == first)
        chip = jnp.where(go_right, right, left)
        slot = jnp.where(go_right, LF, RT)
        dirs.append([rc(kv_send.at[hh, pl.ds(blk * seg, seg), :],
                        kvbuf.at[slot, blk, pl.ds(off(blk, h), seg), :],
                        kvs.at[first, hh, blk], kvr.at[slot, h, blk], chip, hh)
                     for hh in range(2) for blk in range(2)])
    for cp in dirs[0]:
        cp.start()
    for cp in kv_sends:
        cp.start()

    def project(dst, src, grp, w_is_q):
        for p in range(groups // 2):
            if w_is_q:
                a = grp * groups + 2 * p
                w = jnp.concatenate([wq_v[a], wq_v[a + 1]], axis=1)
                r = dot(src[...], w).astype(BF)
            else:
                w = wo_v[pl.ds(pl.multiple_of((grp * groups + 2 * p) * hd, hd), 2 * hd), :]
                r = dot_nt(src[...], w).astype(BF)
            for k in range(2):
                dst(2 * p + k, r[:, k * hd:(k + 1) * hd])

    def to_send(buf):
        def put(g, val):
            buf[g] = val
        return put

    def to_own(buf):
        def put(g, val):
            for t in range(2):
                buf[t, g, pl.ds(off(t, h), seg), :] = val[t * seg:(t + 1) * seg]
        return put

    def xsends(buf, dst, k):
        return [rc(buf.at[:, pl.ds(t * seg, seg), :], dst.at[t, :, pl.ds(off(t, h), seg), :],
                   qs.at[k, t], qr.at[k, t], c, ho) for t in range(2)]

    loads[3].wait()
    project(to_send(q_send), x_v, ho, True)
    q_sends = xsends(q_send, qbuf, 0)
    for cp in q_sends:
        cp.start()
    for cp in dirs[1]:
        cp.start()
    project(to_own(qbuf), x_v, h, True)
    loads[4].wait()
    loads[5].wait()
    project(to_send(do_send), dy_v, ho, False)
    do_sends = xsends(do_send, dobuf, 1)
    for cp in do_sends:
        cp.start()

    relays = []
    for core, slot, chip in ((0, LF, right), (1, RT, left)):
        for blk in range(2):
            view = kvbuf.at[slot, blk, pl.ds(off(blk, core), seg), :]
            rc(view, view, kvs.at[0, 0, blk], kvr.at[slot, core, blk], chip, h).wait_recv()
            cp = rc(view, kvbuf.at[OP, blk, pl.ds(off(blk, core), seg), :],
                    kvrs.at[core, blk], kvr.at[OP, core, blk], chip, h)
            cp.start()
            relays.append(cp)

    project(to_own(dobuf), dy_v, h, False)

    def fwd(ent, t, slot, blk, diag, init):
        kv = kvbuf[slot, blk]
        k, v = kv[:, :hd], kv[:, hd:]
        for g in range(groups):
            s = dot_nt(k, qbuf[t, g]) * scale2
            dp = dot_nt(v, dobuf[t, g])
            if diag:
                key_pos = lax.broadcasted_iota(jnp.int32, s.shape, 0)
                q_pos = lax.broadcasted_iota(jnp.int32, s.shape, 1)
                s = jnp.where(key_pos > q_pos, -jnp.inf, s)
            m = jnp.max(s, axis=0, keepdims=True)
            if not init:
                m_old = m_run[t, g]
                m = jnp.maximum(m, m_old)
            e = jnp.exp2(s - m)
            l = jnp.sum(e, axis=0, keepdims=True)
            d = jnp.sum(e * dp, axis=0, keepdims=True)
            if not init:
                alpha = jnp.exp2(m_old - m)
                l = l_run[t, g] * alpha + l
                d = d_run[t, g] * alpha + d
            est[ent, g] = e
            dpst[ent, g] = dp
            m_ent[ent, g] = m
            m_run[t, g] = m
            l_run[t, g] = l
            d_run[t, g] = d

    def wait_kv(slot, core, blk):
        view = kvbuf.at[slot, blk, pl.ds(off(blk, core), seg), :]
        rc(view, view, kvs.at[0, 0, 0], kvr.at[slot, core, blk], left, h).wait_recv()

    for k, dst in enumerate((qbuf, dobuf)):
        for t in range(2):
            view = dst.at[t, :, pl.ds(off(t, ho), seg), :]
            rc(view, view, qs.at[k, t], qr.at[k, t], c, ho).wait_recv()
    for blk in range(2):
        wait_kv(OWN, ho, blk)
    fwd(0, 0, OWN, 0, True, True)
    fwd(1, 1, OWN, 1, True, True)
    fwd(2, 1, OWN, 0, False, False)

    def owner_of(slot):
        return jnp.where(slot == LF, left, jnp.where(slot == RT, right, opp))

    def fwd_body(i, carry):
        slot = i + 1

        @pl.when(i == 0)
        def _():
            for blk in range(2):
                wait_kv(LF, 1, blk)

        @pl.when(i == 1)
        def _():
            for blk in range(2):
                wait_kv(RT, 0, blk)

        @pl.when(i == 2)
        def _():
            for core in range(2):
                for blk in range(2):
                    wait_kv(OP, core, blk)

        later = (owner_of(slot) > c).astype(jnp.int32)
        fwd(3 + 2 * i, 1, slot, 0, False, False)
        fwd(4 + 2 * i, later, slot, later, False, False)
        return carry

    lax.fori_loop(0, 3, fwd_body, 0)

    for t in range(2):
        for g in range(groups):
            l = l_run[t, g]
            d_run[t, g] = d_run[t, g] / l
            m_run[t, g] = m_run[t, g] + jnp.log2(l)

    dqt[...] = jnp.zeros_like(dqt)

    def bwd(ent, t, slot, blk):
        for g in range(groups):
            w = jnp.exp2(m_ent[ent, g] - m_run[t, g])
            p = (est[ent, g] * w).astype(BF)
            p_buf[:, g * blk_len:(g + 1) * blk_len] = p
            ds_buf[:, g * blk_len:(g + 1) * blk_len] = (
                p.astype(F32) * (dpst[ent, g] - d_run[t, g])).astype(BF)
        kt = kvbuf[slot, blk][:, :hd].T
        dqt[t] += dot(kt, ds_buf[...])
        dk = dot(ds_buf[...], qbuf[t].reshape(groups * blk_len, hd))
        dv = dot(p_buf[...], dobuf[t].reshape(groups * blk_len, hd))
        return dk, dv

    def put(ref, pair):
        ref[:, :hd] = pair[0]
        ref[:, hd:] = pair[1]

    def add(ref, pair):
        ref[:, :hd] += pair[0]
        ref[:, hd:] += pair[1]

    def half(ref, blk, k):
        return ref.at[blk, pl.ds(k * seg, seg), :]

    def m2copy(slot, blk, k):
        chip = right if slot == RT else left
        side = 0 if slot == RT else 1
        core = k if blk == 0 else 1 - k
        return rc(half(pacc.at[slot], blk, k), fin.at[side, h, blk], m2s.at[side, blk, k],
                  m2r.at[side, h, blk], chip, core)

    m1_copies = []
    for blk in range(2):
        m1_copies.append(rc(half(pacc.at[OP], blk, 0), m1_lf.at[blk], m1s.at[0, blk], m1r.at[0, blk], right, h))
        m1_copies.append(rc(half(pacc.at[OP], blk, 1), m1_rt.at[blk], m1s.at[1, blk], m1r.at[1, blk], left, h))

    def bwd_body(i, carry):
        slot = lax.rem(i + 2, 3) + 1
        later = owner_of(slot) > c
        t2 = later.astype(jnp.int32)
        put(pacc.at[slot, 0], bwd(1 + 2 * slot, 1, slot, 0))
        pair = bwd(2 + 2 * slot, t2, slot, t2)

        @pl.when(later)
        def _():
            put(pacc.at[slot, 1], pair)

        @pl.when(jnp.logical_not(later))
        def _():
            add(pacc.at[slot, 0], pair)
            pacc[slot, 1] = jnp.zeros(pacc.shape[2:], F32)

        @pl.when(i == 0)
        def _():
            for cp in m1_copies:
                cp.start()

        @pl.when(i == 1)
        def _():
            for blk in range(2):
                m2copy(LF, blk, 0).start()

        @pl.when(i == 2)
        def _():
            for blk in range(2):
                m2copy(RT, blk, 1).start()
        return carry

    lax.fori_loop(0, 3, bwd_body, 0)
    put(pown.at[0], bwd(0, 0, OWN, 0))
    put(pown.at[1], bwd(1, 1, OWN, 1))
    add(pown.at[0], bwd(2, 1, OWN, 0))

    fo_copies = []
    for blk in range(2):
        src = pown.at[blk, pl.ds(off(blk, ho), seg), :]
        cp = rc(src, fin_own.at[blk], fos.at[0, blk], fos.at[1, blk], c, ho)
        cp.start()
        fo_copies.append(cp)

    for t in range(2):
        for g in range(groups):
            dq = (dqt[t, :, g * blk_len:(g + 1) * blk_len] * scale).astype(BF).T
            dq_tmp[g] = dq
        for g in range(groups):
            dq_send[g, t * seg:(t + 1) * seg, :] = dq_tmp[g, pl.ds(off(t, ho), seg), :]
            dq_rows[h * groups + g, t * seg:(t + 1) * seg, :] = dq_tmp[g, pl.ds(off(t, h), seg), :]
    dq_copy = rc(dq_send, dq_rows.at[pl.ds(h * groups, groups)], dqs, dqr, c, ho)
    dq_copy.start()

    for blk in range(2):
        for side, buf, slot in ((0, m1_lf, RT), (1, m1_rt, LF)):
            rc(buf.at[blk], buf.at[blk], m1s.at[side, blk], m1r.at[side, blk], left, h).wait_recv()
            pacc[slot, blk, side * seg:(side + 1) * seg, :] += buf[blk]
            m2copy(slot, blk, side).start()

    view = dq_rows.at[pl.ds(ho * groups, groups)]
    rc(dq_send, view, dqs, dqr, c, ho).wait_recv()
    for p in range(groups):
        a = 2 * p
        lhs = jnp.concatenate([dq_rows[a], dq_rows[a + 1]], axis=1)
        w = jnp.concatenate([wq_v[a], wq_v[a + 1]], axis=1)
        r = dot_nt(lhs, w)
        if p == 0:
            acc[...] = r
        else:
            acc[...] += r

    for blk in range(2):
        rc(fin_own.at[blk], fin_own.at[blk], fos.at[0, blk], fos.at[1, blk], c, ho).wait_recv()
        for side in range(2):
            for hh in range(2):
                dst = fin.at[side, hh, blk]
                rc(dst, dst, m2s.at[0, 0, 0], m2r.at[side, hh, blk], left, hh).wait_recv()
    for blk in range(2):
        r = pl.ds(blk * seg, seg)
        for hh, loc in ((h, pown[blk, pl.ds(off(blk, h), seg), :]), (ho, fin_own[blk])):
            tot = fin[0, hh, blk] + fin[1, hh, blk] + loc
            dkv[hh, r, :hd] = (tot[:, :hd] * scale).astype(BF)
            dkv[hh, r, hd:] = tot[:, hd:].astype(BF)
    out_v[...] = (acc[...] + dot_nt(dkv[0], wkv_v[0]) + dot_nt(dkv[1], wkv_v[1])).astype(BF)
    st = pltpu.make_async_copy(out_v, out_hbm, st_sem)
    st.start()

    for cp in kv_sends + dirs[0] + dirs[1] + q_sends + do_sends + relays + m1_copies + fo_copies + [dq_copy]:
        cp.wait_send()
    for slot in (LF, RT):
        for blk in range(2):
            for k in range(2):
                m2copy(slot, blk, k).wait_send()
    st.wait()


def solution(mesh):
    n_dev = mesh.shape["cp"]
    row_spec = P(("dp", "cp"), None)

    def device_fn(x_in, d_y, w_q, w_k, w_v, w_o):
        rows, d_model = x_in.shape
        q_heads, hd = w_q.shape[1], w_q.shape[2]
        kv_heads = w_k.shape[1]
        groups = q_heads // kv_heads
        seg = rows // 2
        blk = rows
        wq_t = jnp.transpose(w_q, (1, 0, 2))
        wk_r = w_k.reshape(d_model * kv_heads, hd)
        wv_r = w_v.reshape(d_model * kv_heads, hd)
        wo_r = w_o.reshape(q_heads * hd, d_model)
        vm = pltpu.VMEM
        dma = pltpu.SemaphoreType.DMA
        scratch = [
            vm((rows, d_model), BF), vm((rows, d_model), BF),
            vm((q_heads, d_model, hd), BF), vm((d_model * kv_heads, hd), BF), vm((d_model * kv_heads, hd), BF),
            vm((q_heads * hd, d_model), BF), vm((d_model * kv_heads, hd), F32), vm((kv_heads, d_model, 2 * hd), BF),
            vm((2, rows, 2 * hd), BF), vm((4, 2, blk, 2 * hd), BF),
            vm((groups, rows, hd), BF), vm((groups, rows, hd), BF),
            vm((2, groups, blk, hd), BF), vm((2, groups, blk, hd), BF),
            vm((9, groups, blk, blk), F32), vm((9, groups, blk, blk), F32),
            vm((2, groups, 1, blk), F32), vm((2, groups, 1, blk), F32), vm((2, groups, 1, blk), F32),
            vm((9, groups, 1, blk), F32),
            vm((blk, groups * blk), BF), vm((blk, groups * blk), BF), vm((2, hd, groups * blk), F32),
            vm((4, 2, blk, 2 * hd), F32), vm((2, blk, 2 * hd), F32),
            vm((2, seg, 2 * hd), F32), vm((2, seg, 2 * hd), F32),
            vm((2, 2, 2, seg, 2 * hd), F32), vm((2, seg, 2 * hd), F32),
            vm((groups, rows, hd), BF), vm((q_heads, rows, hd), BF), vm((rows, d_model), F32), vm((rows, d_model), BF),
            vm((2, rows, 2 * hd), BF), vm((groups, blk, hd), BF),
            dma((6,)), dma, dma((2, 2, 2)), dma((4, 2, 2)), dma((2,)), dma((2, 2)), dma((2, 2)), dma((2, 2)),
            dma((2, 2)), dma((2, 2)), dma((2, 2, 2)), dma((2, 2, 2)), dma((2, 2)), dma, dma,
        ]
        return pl.pallas_call(
            functools.partial(kernel, n_dev),
            out_shape=jax.ShapeDtypeStruct((rows, d_model), BF),
            in_specs=[pl.BlockSpec(memory_space=pl.ANY)] * 6,
            out_specs=pl.BlockSpec(memory_space=pl.ANY),
            scratch_shapes=scratch,
            compiler_params=pltpu.CompilerParams(collective_id=0, has_side_effects=True, vmem_limit_bytes=62 * 1024 * 1024),
        )(x_in, d_y, wq_t, wk_r, wv_r, wo_r)

    return jax.shard_map(device_fn, mesh=mesh, in_specs=(row_spec, row_spec, P(), P(), P(), P()), out_specs=row_spec, check_vma=False)
```

```python
import functools
import math

import jax
import jax.numpy as jnp
from jax import lax
from jax.experimental import pallas as pl
from jax.experimental.pallas import tpu as pltpu
from jax.sharding import PartitionSpec as P

MESH = pl.DeviceIdType.MESH
BF = jnp.bfloat16
F32 = jnp.float32
OWN, LF, RT, OP = 0, 1, 2, 3
NT = (((1,), (1,)), ((), ()))


def dot(a, b):
    return jnp.dot(a, b, preferred_element_type=F32)


def dot_nt(a, b):
    return lax.dot_general(a, b, NT, preferred_element_type=F32)


def kernel(n_dev, x_hbm, dy_hbm, wq_hbm, wk_hbm, wv_hbm, wo_hbm, out_v,
           x_v, dy_v, wq_v, wk_v, wv_v, wo_v, wf_v, wkv_v,
           kv_send, kvbuf, q_send, do_send, qbuf, dobuf,
           est, dpst, m_run, l_run, d_run, m_ent, p_buf, ds_buf, dqt,
           pacc, pown, m1_lf, m1_rt, fin, fin_own, dq_send, dq_rows, acc, dkv, dq_tmp, wkvt,
           ld_sem, kvs, kvr, kvps, kvrs, qs, qr, m1s, m1r, m2s, m2r, fos, dqs, dqr):
    me = lax.axis_index("cp")
    n_chip = n_dev // 2
    c = me // 2
    h = me % 2
    ho = 1 - h
    right = lax.rem(c + 1, n_chip)
    left = lax.rem(c + n_chip - 1, n_chip)
    opp = lax.rem(c + 2, n_chip)
    rows, d_model = x_v.shape
    seg = rows // 2
    blk_len = kvbuf.shape[2]
    hd = qbuf.shape[3]
    groups = qbuf.shape[1]
    scale = hd ** -0.5
    scale2 = scale * math.log2(math.e)

    def off(blk, core):
        r = core if blk == 0 else 1 - core
        return pl.multiple_of(r * seg, seg)

    def rc(src, dst, ssem, rsem, chip, core):
        return pltpu.make_async_remote_copy(src_ref=src, dst_ref=dst, send_sem=ssem, recv_sem=rsem,
                                            device_id={"cp": chip * 2 + core}, device_id_type=MESH)

    loads = [pltpu.make_async_copy(a, b, ld_sem.at[i]) for i, (a, b) in enumerate([
        (wk_hbm, wk_v), (wv_hbm, wv_v), (x_hbm, x_v), (wq_hbm, wq_v), (dy_hbm, dy_v), (wo_hbm, wo_v)])]
    for cp in loads[:3]:
        cp.start()

    barrier = pltpu.get_barrier_semaphore()
    for chip, core in ((c, ho), (right, 0), (right, 1), (left, 0), (left, 1)):
        pl.semaphore_signal(barrier, inc=1, device_id={"cp": chip * 2 + core}, device_id_type=MESH)

    for j, (ld, w) in enumerate(((loads[0], wk_v), (loads[1], wv_v))):
        ld.wait()
        wf_v[...] = w[...].astype(F32)
        for hh in range(2):
            wkv_v[hh, :, j * hd:(j + 1) * hd] = wf_v[pl.ds(hh, d_model, stride=2), :].astype(BF)
    loads[2].wait()
    for cp in loads[3:]:
        cp.start()
    for hh in range(2):
        kv_send[hh] = dot(x_v[...], wkv_v[hh]).astype(BF)
    for blk in range(2):
        kvbuf[OWN, blk, pl.ds(off(blk, h), seg), :] = kv_send[h, blk * seg:(blk + 1) * seg, :]

    pl.semaphore_wait(barrier, 5)

    kv_sends = []
    for blk in range(2):
        kv_sends.append(rc(kv_send.at[ho, pl.ds(blk * seg, seg), :],
                           kvbuf.at[OWN, blk, pl.ds(off(blk, h), seg), :],
                           kvps.at[blk], kvr.at[OWN, h, blk], c, ho))
    def kv_copies(d, hh):
        go_right = (h == d)
        chip = jnp.where(go_right, right, left)
        slot = jnp.where(go_right, LF, RT)
        return [rc(kv_send.at[hh, pl.ds(blk * seg, seg), :],
                   kvbuf.at[slot, blk, pl.ds(off(blk, h), seg), :],
                   kvs.at[d, hh, blk], kvr.at[slot, h, blk], chip, hh) for blk in range(2)]

    dirs = [kv_copies(0, 0), kv_copies(1, 0), kv_copies(0, 1), kv_copies(1, 1)]
    for cp in dirs[0] + dirs[1] + dirs[2] + kv_sends:
        cp.start()

    def project(dst, src, grp, w_is_q):
        for p in range(groups // 2):
            if w_is_q:
                a = grp * groups + 2 * p
                w = jnp.concatenate([wq_v[a], wq_v[a + 1]], axis=1)
                r = dot(src[...], w).astype(BF)
            else:
                w = wo_v[pl.ds(pl.multiple_of((grp * groups + 2 * p) * hd, hd), 2 * hd), :]
                r = dot_nt(src[...], w).astype(BF)
            for k in range(2):
                dst(2 * p + k, r[:, k * hd:(k + 1) * hd])

    def to_send(buf):
        def put(g, val):
            buf[g] = val
        return put

    def to_own(buf):
        def put(g, val):
            for t in range(2):
                buf[t, g, pl.ds(off(t, h), seg), :] = val[t * seg:(t + 1) * seg]
        return put

    def xsends(buf, dst, k):
        return [rc(buf.at[:, pl.ds(t * seg, seg), :], dst.at[t, :, pl.ds(off(t, h), seg), :],
                   qs.at[k, t], qr.at[k, t], c, ho) for t in range(2)]

    loads[3].wait()
    project(to_send(q_send), x_v, ho, True)
    q_sends = xsends(q_send, qbuf, 0)
    for cp in q_sends:
        cp.start()
    project(to_own(qbuf), x_v, h, True)
    loads[4].wait()
    loads[5].wait()
    project(to_send(do_send), dy_v, ho, False)
    do_sends = xsends(do_send, dobuf, 1)
    for cp in do_sends:
        cp.start()

    def relay(start):
        cps = []
        for core, slot, chip in ((0, LF, right), (1, RT, left)):
            for blk in range(2):
                view = kvbuf.at[slot, blk, pl.ds(off(blk, core), seg), :]
                cp = rc(view, kvbuf.at[OP, blk, pl.ds(off(blk, core), seg), :],
                        kvrs.at[core, blk], kvr.at[OP, core, blk], chip, h)
                if start:
                    rc(view, view, kvs.at[0, 0, blk], kvr.at[slot, core, blk], chip, h).wait_recv()
                    cp.start()
                cps.append(cp)
        return cps

    project(to_own(dobuf), dy_v, h, False)

    @pl.when(h == 0)
    def _():
        relay(True)

    def fwd(ent, t, slot, blk, diag, init):
        kv = kvbuf[slot, blk]
        k, v = kv[:, :hd], kv[:, hd:]
        for g in range(groups):
            s = dot_nt(k, qbuf[t, g]) * scale2
            dp = dot_nt(v, dobuf[t, g])
            if diag:
                key_pos = lax.broadcasted_iota(jnp.int32, s.shape, 0)
                q_pos = lax.broadcasted_iota(jnp.int32, s.shape, 1)
                s = jnp.where(key_pos > q_pos, -jnp.inf, s)
            m = jnp.max(s, axis=0, keepdims=True)
            if not init:
                m_old = m_run[t, g]
                m = jnp.maximum(m, m_old)
            e = jnp.exp2(s - m)
            l = jnp.sum(e, axis=0, keepdims=True)
            d = jnp.sum(e * dp, axis=0, keepdims=True)
            if not init:
                alpha = jnp.exp2(m_old - m)
                l = l_run[t, g] * alpha + l
                d = d_run[t, g] * alpha + d
            est[ent, g] = e
            dpst[ent, g] = dp
            m_ent[ent, g] = m
            m_run[t, g] = m
            l_run[t, g] = l
            d_run[t, g] = d

    def wait_kv(slot, core, blk):
        view = kvbuf.at[slot, blk, pl.ds(off(blk, core), seg), :]
        rc(view, view, kvs.at[0, 0, 0], kvr.at[slot, core, blk], left, h).wait_recv()

    for k, dst in enumerate((qbuf, dobuf)):
        for t in range(2):
            view = dst.at[t, :, pl.ds(off(t, ho), seg), :]
            rc(view, view, qs.at[k, t], qr.at[k, t], c, ho).wait_recv()
    for blk in range(2):
        wait_kv(OWN, ho, blk)
    m_run[0] = jnp.full(m_run.shape[1:], -jnp.inf, F32)
    l_run[0] = jnp.zeros(l_run.shape[1:], F32)
    d_run[0] = jnp.zeros(d_run.shape[1:], F32)
    fwd(1, 1, OWN, 1, True, True)
    fwd(2, 1, OWN, 0, False, False)
    for cp in dirs[3]:
        cp.start()

    @pl.when(h == 1)
    def _():
        relay(True)

    def owner_of(slot):
        return jnp.where(slot == LF, left, jnp.where(slot == RT, right, opp))

    def fwd_body(i, carry):
        slot = i + 1

        @pl.when(i == 0)
        def _():
            for blk in range(2):
                wait_kv(LF, 1, blk)

        @pl.when(i == 1)
        def _():
            for blk in range(2):
                wait_kv(RT, 0, blk)

        @pl.when(i == 2)
        def _():
            fwd(0, 0, OWN, 0, True, False)
            for core in range(2):
                for blk in range(2):
                    wait_kv(OP, core, blk)

        later = (owner_of(slot) > c).astype(jnp.int32)
        fwd(3 + 2 * i, 1, slot, 0, False, False)
        fwd(4 + 2 * i, later, slot, later, False, False)
        return carry

    lax.fori_loop(0, 3, fwd_body, 0)

    for t in range(2):
        for g in range(groups):
            l = l_run[t, g]
            d_run[t, g] = d_run[t, g] / l
            m_run[t, g] = m_run[t, g] + jnp.log2(l)

    dqt[...] = jnp.zeros_like(dqt)

    def bwd(ent, t, slot, blk):
        for g in range(groups):
            w = jnp.exp2(m_ent[ent, g] - m_run[t, g])
            p = (est[ent, g] * w).astype(BF)
            p_buf[:, g * blk_len:(g + 1) * blk_len] = p
            ds_buf[:, g * blk_len:(g + 1) * blk_len] = (
                p.astype(F32) * (dpst[ent, g] - d_run[t, g])).astype(BF)
        kt = kvbuf[slot, blk][:, :hd].T
        dqt[t] += dot(kt, ds_buf[...])
        dk = dot(ds_buf[...], qbuf[t].reshape(groups * blk_len, hd))
        dv = dot(p_buf[...], dobuf[t].reshape(groups * blk_len, hd))
        return dk, dv

    def put(ref, pair):
        ref[:, :hd] = pair[0]
        ref[:, hd:] = pair[1]

    def add(ref, pair):
        ref[:, :hd] += pair[0]
        ref[:, hd:] += pair[1]

    def half(ref, blk, k):
        return ref.at[blk, pl.ds(k * seg, seg), :]

    def has(o, *chips):
        return functools.reduce(jnp.logical_or, [o > x for x in chips])

    def when(blk, cond, f):
        if blk == 0:
            f()
        else:
            pl.when(cond)(f)

    def m2copy(slot, blk, k):
        chip = right if slot == RT else left
        side = 0 if slot == RT else 1
        core = k if blk == 0 else 1 - k
        return rc(half(pacc.at[slot], blk, k), fin.at[side, h, blk], m2s.at[side, blk, k],
                  m2r.at[side, h, blk], chip, core)

    m1_copies = []
    for blk in range(2):
        m1_copies.append(rc(half(pacc.at[OP], blk, 0), m1_lf.at[blk], m1s.at[0, blk], m1r.at[0, blk], right, h))
        m1_copies.append(rc(half(pacc.at[OP], blk, 1), m1_rt.at[blk], m1s.at[1, blk], m1r.at[1, blk], left, h))

    def bwd_body(i, carry):
        slot = lax.rem(i + 2, 3) + 1
        later = owner_of(slot) > c
        t2 = later.astype(jnp.int32)
        put(pacc.at[slot, 0], bwd(1 + 2 * slot, 1, slot, 0))

        @pl.when(jnp.logical_and(i == 0, later))
        def _():
            for cp in m1_copies[:2]:
                cp.start()

        pair = bwd(2 + 2 * slot, t2, slot, t2)

        @pl.when(later)
        def _():
            put(pacc.at[slot, 1], pair)

        @pl.when(jnp.logical_not(later))
        def _():
            add(pacc.at[slot, 0], pair)
            pacc[slot, 1] = jnp.zeros(pacc.shape[2:], F32)

        @pl.when(i == 0)
        def _():
            @pl.when(later)
            def _():
                for cp in m1_copies[2:]:
                    cp.start()

            @pl.when(jnp.logical_not(later))
            def _():
                for cp in m1_copies[:2]:
                    cp.start()

        @pl.when(i == 1)
        def _():
            for blk in range(2):
                when(blk, has(left, c), lambda: m2copy(LF, blk, 0).start())

        @pl.when(i == 2)
        def _():
            for blk in range(2):
                when(blk, has(right, c), lambda: m2copy(RT, blk, 1).start())
        return carry

    lax.fori_loop(0, 3, bwd_body, 0)
    put(pown.at[0], bwd(0, 0, OWN, 0))
    put(pown.at[1], bwd(1, 1, OWN, 1))
    add(pown.at[0], bwd(2, 1, OWN, 0))

    fo_copies = []
    for blk in range(2):
        src = pown.at[blk, pl.ds(off(blk, ho), seg), :]
        cp = rc(src, fin_own.at[blk], fos.at[0, blk], fos.at[1, blk], c, ho)
        cp.start()
        fo_copies.append(cp)

    for t in range(2):
        for g in range(groups):
            dq = (dqt[t, :, g * blk_len:(g + 1) * blk_len] * scale).astype(BF).T
            dq_tmp[g] = dq
        for g in range(groups):
            dq_send[g, t * seg:(t + 1) * seg, :] = dq_tmp[g, pl.ds(off(t, ho), seg), :]
            dq_rows[h * groups + g, t * seg:(t + 1) * seg, :] = dq_tmp[g, pl.ds(off(t, h), seg), :]
    dq_copy = rc(dq_send, dq_rows.at[pl.ds(h * groups, groups)], dqs, dqr, c, ho)
    dq_copy.start()

    for blk in range(2):
        for side, buf, slot, o, s in ((0, m1_lf, RT, right, left), (1, m1_rt, LF, left, right)):
            def f():
                rc(buf.at[blk], buf.at[blk], m1s.at[side, blk], m1r.at[side, blk], left, h).wait_recv()
                pacc[slot, blk, side * seg:(side + 1) * seg, :] += buf[blk]
            when(blk, has(o, s), f)
            when(blk, has(o, s, c), lambda: m2copy(slot, blk, side).start())

    view = dq_rows.at[pl.ds(ho * groups, groups)]
    rc(dq_send, view, dqs, dqr, c, ho).wait_recv()
    for p in range(groups):
        a = 2 * p
        lhs = jnp.concatenate([dq_rows[a], dq_rows[a + 1]], axis=1)
        w = jnp.concatenate([wq_v[a], wq_v[a + 1]], axis=1)
        r = dot_nt(lhs, w)
        if p == 0:
            acc[...] = r
        else:
            acc[...] += r

    for hh in range(2):
        wkvt[hh] = wkv_v[hh].T

    for blk in range(2):
        rc(fin_own.at[blk], fin_own.at[blk], fos.at[0, blk], fos.at[1, blk], c, ho).wait_recv()
        for side, s in ((0, left), (1, right)):
            merged = (h if blk == 0 else 1 - h) == side
            arrives = jnp.logical_or(has(c, s), jnp.logical_and(merged, has(c, opp)))
            for hh in range(2):
                def f():
                    dst = fin.at[side, hh, blk]
                    rc(dst, dst, m2s.at[0, 0, 0], m2r.at[side, hh, blk], left, hh).wait_recv()
                when(blk, arrives, f)
                if blk == 1:
                    @pl.when(jnp.logical_not(arrives))
                    def _():
                        fin[side, hh, blk] = jnp.zeros(fin.shape[3:], F32)
    for blk in range(2):
        r = pl.ds(blk * seg, seg)
        for hh, loc in ((h, pown[blk, pl.ds(off(blk, h), seg), :]), (ho, fin_own[blk])):
            tot = fin[0, hh, blk] + fin[1, hh, blk] + loc
            dkv[hh, r, :hd] = (tot[:, :hd] * scale).astype(BF)
            dkv[hh, r, hd:] = tot[:, hd:].astype(BF)
    out_v[...] = (acc[...] + dot(dkv[0], wkvt[0]) + dot(dkv[1], wkvt[1])).astype(BF)

    for cp in kv_sends + sum(dirs, []) + q_sends + do_sends + relay(False) + fo_copies + [dq_copy]:
        cp.wait_send()
    for blk in range(2):
        def f():
            for cp in m1_copies[2 * blk:2 * blk + 2]:
                cp.wait_send()
        when(blk, has(opp, c), f)
        for slot, o, s, side in ((RT, right, left, 0), (LF, left, right, 1)):
            when(blk, has(o, s, c), lambda: m2copy(slot, blk, side).wait_send())
            when(blk, has(o, c), lambda: m2copy(slot, blk, 1 - side).wait_send())


def solution(mesh):
    n_dev = mesh.shape["cp"]
    row_spec = P(("dp", "cp"), None)

    def device_fn(x_in, d_y, w_q, w_k, w_v, w_o):
        rows, d_model = x_in.shape
        q_heads, hd = w_q.shape[1], w_q.shape[2]
        kv_heads = w_k.shape[1]
        groups = q_heads // kv_heads
        seg = rows // 2
        blk = rows
        wq_t = jnp.transpose(w_q, (1, 0, 2))
        wk_r = w_k.reshape(d_model * kv_heads, hd)
        wv_r = w_v.reshape(d_model * kv_heads, hd)
        wo_r = w_o.reshape(q_heads * hd, d_model)
        vm = pltpu.VMEM
        dma = pltpu.SemaphoreType.DMA
        scratch = [
            vm((rows, d_model), BF), vm((rows, d_model), BF),
            vm((q_heads, d_model, hd), BF), vm((d_model * kv_heads, hd), BF), vm((d_model * kv_heads, hd), BF),
            vm((q_heads * hd, d_model), BF), vm((d_model * kv_heads, hd), F32), vm((kv_heads, d_model, 2 * hd), BF),
            vm((2, rows, 2 * hd), BF), vm((4, 2, blk, 2 * hd), BF),
            vm((groups, rows, hd), BF), vm((groups, rows, hd), BF),
            vm((2, groups, blk, hd), BF), vm((2, groups, blk, hd), BF),
            vm((9, groups, blk, blk), F32), vm((9, groups, blk, blk), F32),
            vm((2, groups, 1, blk), F32), vm((2, groups, 1, blk), F32), vm((2, groups, 1, blk), F32),
            vm((9, groups, 1, blk), F32),
            vm((blk, groups * blk), BF), vm((blk, groups * blk), BF), vm((2, hd, groups * blk), F32),
            vm((4, 2, blk, 2 * hd), F32), vm((2, blk, 2 * hd), F32),
            vm((2, seg, 2 * hd), F32), vm((2, seg, 2 * hd), F32),
            vm((2, 2, 2, seg, 2 * hd), F32), vm((2, seg, 2 * hd), F32),
            vm((groups, rows, hd), BF), vm((q_heads, rows, hd), BF), vm((rows, d_model), F32),
            vm((2, rows, 2 * hd), BF), vm((groups, blk, hd), BF), vm((kv_heads, 2 * hd, d_model), BF),
            dma((6,)), dma((2, 2, 2)), dma((4, 2, 2)), dma((2,)), dma((2, 2)), dma((2, 2)), dma((2, 2)),
            dma((2, 2)), dma((2, 2)), dma((2, 2, 2)), dma((2, 2, 2)), dma((2, 2)), dma, dma,
        ]
        res = pl.pallas_call(
            functools.partial(kernel, n_dev),
            out_shape=pltpu.VMEM((rows, d_model), BF),
            in_specs=[pl.BlockSpec(memory_space=pl.ANY)] * 6,
            out_specs=pl.BlockSpec(memory_space=pltpu.VMEM),
            scratch_shapes=scratch,
            compiler_params=pltpu.CompilerParams(collective_id=0, has_side_effects=True, vmem_limit_bytes=62 * 1024 * 1024),
        )(x_in, d_y, wq_t, wk_r, wv_r, wo_r)
        return res

    return jax.shard_map(device_fn, mesh=mesh, in_specs=(row_spec, row_spec, P(), P(), P(), P()), out_specs=row_spec, check_vma=False)
```

```python
import functools
import math

import jax
import jax.numpy as jnp
from jax import lax
from jax.experimental import pallas as pl
from jax.experimental.pallas import tpu as pltpu
from jax.sharding import PartitionSpec as P

MESH = pl.DeviceIdType.MESH
BF = jnp.bfloat16
F32 = jnp.float32
OWN, LF, RT, OP = 0, 1, 2, 3
NT = (((1,), (1,)), ((), ()))


def dot(a, b):
    return jnp.dot(a, b, preferred_element_type=F32)


def dot_nt(a, b):
    return lax.dot_general(a, b, NT, preferred_element_type=F32)


def kernel(n_dev, x_hbm, dy_hbm, wq_hbm, wk_hbm, wv_hbm, wo_hbm, out_v,
           x_v, dy_v, wq_v, wk_v, wv_v, wo_v, wf_v, wkv_v,
           kv_send, kvbuf, q_send, do_send, qbuf, dobuf,
           est, dpst, m_run, l_run, d_run, m_ent, p_buf, ds_buf, dqt,
           pacc, pown, m1_lf, m1_rt, fin, fin_own, dq_send, dq_rows, acc, dkv, dq_tmp, wkvt,
           ld_sem, kvs, kvr, kvps, kvrs, qs, qr, m1s, m1r, m2s, m2r, fos, dqs, dqr):
    me = lax.axis_index("cp")
    n_chip = n_dev // 2
    c = me // 2
    h = me % 2
    ho = 1 - h
    right = lax.rem(c + 1, n_chip)
    left = lax.rem(c + n_chip - 1, n_chip)
    opp = lax.rem(c + 2, n_chip)
    rows, d_model = x_v.shape
    seg = rows // 2
    blk_len = kvbuf.shape[2]
    hd = qbuf.shape[3]
    groups = qbuf.shape[1]
    scale = hd ** -0.5
    scale2 = scale * math.log2(math.e)

    def off(blk, core):
        r = core if blk == 0 else 1 - core
        return pl.multiple_of(r * seg, seg)

    def rc(src, dst, ssem, rsem, chip, core):
        return pltpu.make_async_remote_copy(src_ref=src, dst_ref=dst, send_sem=ssem, recv_sem=rsem,
                                            device_id={"cp": chip * 2 + core}, device_id_type=MESH)

    def load(i, src, dst):
        return pltpu.make_async_copy(src, dst, ld_sem.at[i])

    ld_k, ld_v, ld_x = load(0, wk_hbm, wk_v), load(1, wv_hbm, wv_v), load(2, x_hbm, x_v)
    ld_q, ld_y, ld_o = load(3, wq_hbm, wq_v), load(4, dy_hbm, dy_v), load(5, wo_hbm, wo_v)
    for cp in (ld_k, ld_v, ld_x, ld_q):
        cp.start()

    barrier = pltpu.get_barrier_semaphore()
    for chip, core in ((c, ho), (right, 0), (right, 1), (left, 0), (left, 1)):
        pl.semaphore_signal(barrier, inc=1, device_id={"cp": chip * 2 + core}, device_id_type=MESH)

    for j, (ld, w) in enumerate(((ld_k, wk_v), (ld_v, wv_v))):
        ld.wait()
        if j == 0:
            for cp in (ld_y, ld_o):
                cp.start()
        wf_v[...] = w[...].astype(F32)
        for hh in range(2):
            wkv_v[hh, :, j * hd:(j + 1) * hd] = wf_v[pl.ds(hh, d_model, stride=2), :].astype(BF)
    ld_x.wait()
    for cp in ():
        cp.start()
    for hh in range(2):
        kv_send[hh] = dot(x_v[...], wkv_v[hh]).astype(BF)
    for blk in range(2):
        kvbuf[OWN, blk, pl.ds(off(blk, h), seg), :] = kv_send[h, blk * seg:(blk + 1) * seg, :]

    pl.semaphore_wait(barrier, 5)

    kv_sends = []
    for blk in range(2):
        kv_sends.append(rc(kv_send.at[ho, pl.ds(blk * seg, seg), :],
                           kvbuf.at[OWN, blk, pl.ds(off(blk, h), seg), :],
                           kvps.at[blk], kvr.at[OWN, h, blk], c, ho))
    def kv_copies(d, hh):
        go_right = (h == d)
        chip = jnp.where(go_right, right, left)
        slot = jnp.where(go_right, LF, RT)
        return [rc(kv_send.at[hh, pl.ds(blk * seg, seg), :],
                   kvbuf.at[slot, blk, pl.ds(off(blk, h), seg), :],
                   kvs.at[d, hh, blk], kvr.at[slot, h, blk], chip, hh) for blk in range(2)]

    dirs = [kv_copies(0, 0), kv_copies(1, 0), kv_copies(0, 1), kv_copies(1, 1)]
    for cp in dirs[0] + dirs[1] + kv_sends:
        cp.start()

    def project(dst, src, grp, w_is_q):
        for p in range(groups // 2):
            if w_is_q:
                a = grp * groups + 2 * p
                w = jnp.concatenate([wq_v[a], wq_v[a + 1]], axis=1)
                r = dot(src[...], w).astype(BF)
            else:
                w = wo_v[pl.ds(pl.multiple_of((grp * groups + 2 * p) * hd, hd), 2 * hd), :]
                r = dot_nt(src[...], w).astype(BF)
            for k in range(2):
                dst(2 * p + k, r[:, k * hd:(k + 1) * hd])

    def to_send(buf):
        def put(g, val):
            buf[g] = val
        return put

    def to_own(buf):
        def put(g, val):
            for t in range(2):
                buf[t, g, pl.ds(off(t, h), seg), :] = val[t * seg:(t + 1) * seg]
        return put

    def xsends(buf, dst, k):
        return [rc(buf.at[:, pl.ds(t * seg, seg), :], dst.at[t, :, pl.ds(off(t, h), seg), :],
                   qs.at[k, t], qr.at[k, t], c, ho) for t in range(2)]

    ld_q.wait()
    project(to_send(q_send), x_v, ho, True)
    q_sends = xsends(q_send, qbuf, 0)
    for cp in q_sends:
        cp.start()
    project(to_own(qbuf), x_v, h, True)
    for cp in dirs[2] + dirs[3]:
        cp.start()
    ld_y.wait()
    ld_o.wait()
    project(to_send(do_send), dy_v, ho, False)
    do_sends = xsends(do_send, dobuf, 1)
    for cp in do_sends:
        cp.start()
    project(to_own(dobuf), dy_v, h, False)

    def relay(start):
        cps = []
        for core, slot, chip in ((0, LF, right), (1, RT, left)):
            for blk in range(2):
                view = kvbuf.at[slot, blk, pl.ds(off(blk, core), seg), :]
                cp = rc(view, kvbuf.at[OP, blk, pl.ds(off(blk, core), seg), :],
                        kvrs.at[core, blk], kvr.at[OP, core, blk], chip, h)
                if start:
                    rc(view, view, kvs.at[0, 0, blk], kvr.at[slot, core, blk], chip, h).wait_recv()
                    cp.start()
                cps.append(cp)
        return cps

    @pl.when(h == 0)
    def _():
        relay(True)

    def fwd(ent, t, slot, blk, diag, init):
        kv = kvbuf[slot, blk]
        k, v = kv[:, :hd], kv[:, hd:]
        for g in range(groups):
            s = dot_nt(k, qbuf[t, g]) * scale2
            dp = dot_nt(v, dobuf[t, g])
            if diag:
                key_pos = lax.broadcasted_iota(jnp.int32, s.shape, 0)
                q_pos = lax.broadcasted_iota(jnp.int32, s.shape, 1)
                s = jnp.where(key_pos > q_pos, -jnp.inf, s)
            m = jnp.max(s, axis=0, keepdims=True)
            if not init:
                m_old = m_run[t, g]
                m = jnp.maximum(m, m_old)
            e = jnp.exp2(s - m)
            l = jnp.sum(e, axis=0, keepdims=True)
            d = jnp.sum(e * dp, axis=0, keepdims=True)
            if not init:
                alpha = jnp.exp2(m_old - m)
                l = l_run[t, g] * alpha + l
                d = d_run[t, g] * alpha + d
            est[ent, g] = e
            dpst[ent, g] = dp
            m_ent[ent, g] = m
            m_run[t, g] = m
            l_run[t, g] = l
            d_run[t, g] = d

    def wait_kv(slot, core, blk):
        view = kvbuf.at[slot, blk, pl.ds(off(blk, core), seg), :]
        rc(view, view, kvs.at[0, 0, 0], kvr.at[slot, core, blk], left, h).wait_recv()

    for k, dst in enumerate((qbuf, dobuf)):
        for t in range(2):
            view = dst.at[t, :, pl.ds(off(t, ho), seg), :]
            rc(view, view, qs.at[k, t], qr.at[k, t], c, ho).wait_recv()
    for blk in range(2):
        wait_kv(OWN, ho, blk)
    m_run[0] = jnp.full(m_run.shape[1:], -jnp.inf, F32)
    l_run[0] = jnp.zeros(l_run.shape[1:], F32)
    d_run[0] = jnp.zeros(d_run.shape[1:], F32)
    fwd(1, 1, OWN, 1, True, True)
    fwd(2, 1, OWN, 0, False, False)
    @pl.when(h == 1)
    def _():
        fwd(0, 0, OWN, 0, True, False)

    @pl.when(h == 1)
    def _():
        relay(True)

    def owner_of(slot):
        return jnp.where(slot == LF, left, jnp.where(slot == RT, right, opp))

    def fwd_body(i, carry):
        slot = i + 1

        @pl.when(i == 0)
        def _():
            for blk in range(2):
                wait_kv(LF, 1, blk)

        @pl.when(i == 1)
        def _():
            for blk in range(2):
                wait_kv(RT, 0, blk)

        @pl.when(i == 2)
        def _():
            for core in range(2):
                for blk in range(2):
                    wait_kv(OP, core, blk)

        later = (owner_of(slot) > c).astype(jnp.int32)
        fwd(3 + 2 * i, 1, slot, 0, False, False)
        fwd(4 + 2 * i, later, slot, later, False, False)
        return carry

    lax.fori_loop(0, 3, fwd_body, 0)

    def finish(t):
        for g in range(groups):
            l = l_run[t, g]
            d_run[t, g] = d_run[t, g] / l
            m_run[t, g] = m_run[t, g] + jnp.log2(l)

    finish(1)

    dqt[...] = jnp.zeros_like(dqt)

    def bwd(ent, t, slot, blk):
        for g in range(groups):
            w = jnp.exp2(m_ent[ent, g] - m_run[t, g])
            p = (est[ent, g] * w).astype(BF)
            p_buf[:, g * blk_len:(g + 1) * blk_len] = p
            ds_buf[:, g * blk_len:(g + 1) * blk_len] = (
                p.astype(F32) * (dpst[ent, g] - d_run[t, g])).astype(BF)
        kt = kvbuf[slot, blk][:, :hd].T
        dqt[t] += dot(kt, ds_buf[...])
        dk = dot(ds_buf[...], qbuf[t].reshape(groups * blk_len, hd))
        dv = dot(p_buf[...], dobuf[t].reshape(groups * blk_len, hd))
        return dk, dv

    def put(ref, pair):
        ref[:, :hd] = pair[0]
        ref[:, hd:] = pair[1]

    def add(ref, pair):
        ref[:, :hd] += pair[0]
        ref[:, hd:] += pair[1]

    def half(ref, blk, k):
        return ref.at[blk, pl.ds(k * seg, seg), :]

    def has(o, *chips):
        return functools.reduce(jnp.logical_or, [o > x for x in chips])

    def when(blk, cond, f):
        if blk == 0:
            f()
        else:
            pl.when(cond)(f)

    def m2copy(slot, blk, k):
        chip = right if slot == RT else left
        side = 0 if slot == RT else 1
        core = k if blk == 0 else 1 - k
        return rc(half(pacc.at[slot], blk, k), fin.at[side, h, blk], m2s.at[side, blk, k],
                  m2r.at[side, h, blk], chip, core)

    m1_copies = []
    for blk in range(2):
        m1_copies.append(rc(half(pacc.at[OP], blk, 0), m1_lf.at[blk], m1s.at[0, blk], m1r.at[0, blk], right, h))
        m1_copies.append(rc(half(pacc.at[OP], blk, 1), m1_rt.at[blk], m1s.at[1, blk], m1r.at[1, blk], left, h))

    def bwd_body(i, carry):
        slot = lax.rem(i + 2, 3) + 1
        later = owner_of(slot) > c
        t2 = later.astype(jnp.int32)
        put(pacc.at[slot, 0], bwd(1 + 2 * slot, 1, slot, 0))

        @pl.when(jnp.logical_and(i == 0, later))
        def _():
            for cp in m1_copies[:2]:
                cp.start()

        @pl.when(i == 0)
        def _():
            @pl.when(h == 0)
            def _():
                fwd(0, 0, OWN, 0, True, False)
            finish(0)

        pair = bwd(2 + 2 * slot, t2, slot, t2)

        @pl.when(later)
        def _():
            put(pacc.at[slot, 1], pair)

        @pl.when(jnp.logical_not(later))
        def _():
            add(pacc.at[slot, 0], pair)
            pacc[slot, 1] = jnp.zeros(pacc.shape[2:], F32)

        @pl.when(i == 0)
        def _():
            @pl.when(later)
            def _():
                for cp in m1_copies[2:]:
                    cp.start()

            @pl.when(jnp.logical_not(later))
            def _():
                for cp in m1_copies[:2]:
                    cp.start()

        @pl.when(i == 1)
        def _():
            for blk in range(2):
                when(blk, has(left, c), lambda: m2copy(LF, blk, 0).start())

        @pl.when(i == 2)
        def _():
            for blk in range(2):
                when(blk, has(right, c), lambda: m2copy(RT, blk, 1).start())
        return carry

    lax.fori_loop(0, 3, bwd_body, 0)
    put(pown.at[0], bwd(0, 0, OWN, 0))
    put(pown.at[1], bwd(1, 1, OWN, 1))
    add(pown.at[0], bwd(2, 1, OWN, 0))

    fo_copies = []
    for blk in range(2):
        src = pown.at[blk, pl.ds(off(blk, ho), seg), :]
        cp = rc(src, fin_own.at[blk], fos.at[0, blk], fos.at[1, blk], c, ho)
        cp.start()
        fo_copies.append(cp)

    for t in range(2):
        for g in range(groups):
            dq = (dqt[t, :, g * blk_len:(g + 1) * blk_len] * scale).astype(BF).T
            dq_tmp[g] = dq
        for g in range(groups):
            dq_send[g, t * seg:(t + 1) * seg, :] = dq_tmp[g, pl.ds(off(t, ho), seg), :]
            dq_rows[h * groups + g, t * seg:(t + 1) * seg, :] = dq_tmp[g, pl.ds(off(t, h), seg), :]
    dq_copy = rc(dq_send, dq_rows.at[pl.ds(h * groups, groups)], dqs, dqr, c, ho)
    dq_copy.start()

    for blk in range(2):
        for side, buf, slot, o, s in ((0, m1_lf, RT, right, left), (1, m1_rt, LF, left, right)):
            def f():
                rc(buf.at[blk], buf.at[blk], m1s.at[side, blk], m1r.at[side, blk], left, h).wait_recv()
                pacc[slot, blk, side * seg:(side + 1) * seg, :] += buf[blk]
            when(blk, has(o, s), f)
            when(blk, has(o, s, c), lambda: m2copy(slot, blk, side).start())

    view = dq_rows.at[pl.ds(ho * groups, groups)]
    rc(dq_send, view, dqs, dqr, c, ho).wait_recv()
    for p in range(groups):
        a = 2 * p
        lhs = jnp.concatenate([dq_rows[a], dq_rows[a + 1]], axis=1)
        w = jnp.concatenate([wq_v[a], wq_v[a + 1]], axis=1)
        r = dot_nt(lhs, w)
        if p == 0:
            acc[...] = r
        else:
            acc[...] += r

    for hh in range(2):
        wkvt[hh] = wkv_v[hh].T

    for blk in range(2):
        rc(fin_own.at[blk], fin_own.at[blk], fos.at[0, blk], fos.at[1, blk], c, ho).wait_recv()
        for side, s in ((0, left), (1, right)):
            merged = (h if blk == 0 else 1 - h) == side
            arrives = jnp.logical_or(has(c, s), jnp.logical_and(merged, has(c, opp)))
            for hh in range(2):
                def f():
                    dst = fin.at[side, hh, blk]
                    rc(dst, dst, m2s.at[0, 0, 0], m2r.at[side, hh, blk], left, hh).wait_recv()
                when(blk, arrives, f)
                if blk == 1:
                    @pl.when(jnp.logical_not(arrives))
                    def _():
                        fin[side, hh, blk] = jnp.zeros(fin.shape[3:], F32)
    for blk in range(2):
        r = pl.ds(blk * seg, seg)
        for hh, loc in ((h, pown[blk, pl.ds(off(blk, h), seg), :]), (ho, fin_own[blk])):
            tot = fin[0, hh, blk] + fin[1, hh, blk] + loc
            dkv[hh, r, :hd] = (tot[:, :hd] * scale).astype(BF)
            dkv[hh, r, hd:] = tot[:, hd:].astype(BF)
    out_v[...] = (acc[...] + dot(dkv[0], wkvt[0]) + dot(dkv[1], wkvt[1])).astype(BF)

    for cp in kv_sends + sum(dirs, []) + q_sends + do_sends + relay(False) + fo_copies + [dq_copy]:
        cp.wait_send()
    for blk in range(2):
        def f():
            for cp in m1_copies[2 * blk:2 * blk + 2]:
                cp.wait_send()
        when(blk, has(opp, c), f)
        for slot, o, s, side in ((RT, right, left, 0), (LF, left, right, 1)):
            when(blk, has(o, s, c), lambda: m2copy(slot, blk, side).wait_send())
            when(blk, has(o, c), lambda: m2copy(slot, blk, 1 - side).wait_send())


def solution(mesh):
    n_dev = mesh.shape["cp"]
    row_spec = P(("dp", "cp"), None)

    def device_fn(x_in, d_y, w_q, w_k, w_v, w_o):
        rows, d_model = x_in.shape
        q_heads, hd = w_q.shape[1], w_q.shape[2]
        kv_heads = w_k.shape[1]
        groups = q_heads // kv_heads
        seg = rows // 2
        blk = rows
        wq_t = jnp.transpose(w_q, (1, 0, 2))
        wk_r = w_k.reshape(d_model * kv_heads, hd)
        wv_r = w_v.reshape(d_model * kv_heads, hd)
        wo_r = w_o.reshape(q_heads * hd, d_model)
        vm = pltpu.VMEM
        dma = pltpu.SemaphoreType.DMA
        scratch = [
            vm((rows, d_model), BF), vm((rows, d_model), BF),
            vm((q_heads, d_model, hd), BF), vm((d_model * kv_heads, hd), BF), vm((d_model * kv_heads, hd), BF),
            vm((q_heads * hd, d_model), BF), vm((d_model * kv_heads, hd), F32), vm((kv_heads, d_model, 2 * hd), BF),
            vm((2, rows, 2 * hd), BF), vm((4, 2, blk, 2 * hd), BF),
            vm((groups, rows, hd), BF), vm((groups, rows, hd), BF),
            vm((2, groups, blk, hd), BF), vm((2, groups, blk, hd), BF),
            vm((9, groups, blk, blk), F32), vm((9, groups, blk, blk), F32),
            vm((2, groups, 1, blk), F32), vm((2, groups, 1, blk), F32), vm((2, groups, 1, blk), F32),
            vm((9, groups, 1, blk), F32),
            vm((blk, groups * blk), BF), vm((blk, groups * blk), BF), vm((2, hd, groups * blk), F32),
            vm((4, 2, blk, 2 * hd), F32), vm((2, blk, 2 * hd), F32),
            vm((2, seg, 2 * hd), F32), vm((2, seg, 2 * hd), F32),
            vm((2, 2, 2, seg, 2 * hd), F32), vm((2, seg, 2 * hd), F32),
            vm((groups, rows, hd), BF), vm((q_heads, rows, hd), BF), vm((rows, d_model), F32),
            vm((2, rows, 2 * hd), BF), vm((groups, blk, hd), BF), vm((kv_heads, 2 * hd, d_model), BF),
            dma((6,)), dma((2, 2, 2)), dma((4, 2, 2)), dma((2,)), dma((2, 2)), dma((2, 2)), dma((2, 2)),
            dma((2, 2)), dma((2, 2)), dma((2, 2, 2)), dma((2, 2, 2)), dma((2, 2)), dma, dma,
        ]
        res = pl.pallas_call(
            functools.partial(kernel, n_dev),
            out_shape=pltpu.VMEM((rows, d_model), BF),
            in_specs=[pl.BlockSpec(memory_space=pl.ANY)] * 6,
            out_specs=pl.BlockSpec(memory_space=pltpu.VMEM),
            scratch_shapes=scratch,
            compiler_params=pltpu.CompilerParams(collective_id=0, has_side_effects=True, vmem_limit_bytes=62 * 1024 * 1024),
        )(x_in, d_y, wq_t, wk_r, wv_r, wo_r)
        return res

    return jax.shard_map(device_fn, mesh=mesh, in_specs=(row_spec, row_spec, P(), P(), P(), P()), out_specs=row_spec, check_vma=False)
```

```python
import functools
import math

import jax
import jax.numpy as jnp
from jax import lax
from jax.experimental import pallas as pl
from jax.experimental.pallas import tpu as pltpu
from jax.sharding import PartitionSpec as P

MESH = pl.DeviceIdType.MESH
BF = jnp.bfloat16
F32 = jnp.float32
OWN, LF, RT, OP = 0, 1, 2, 3
MERGE_EARLY = True
NT = (((1,), (1,)), ((), ()))


def dot(a, b):
    return jnp.dot(a, b, preferred_element_type=F32)


def dot_nt(a, b):
    return lax.dot_general(a, b, NT, preferred_element_type=F32)


def kernel(n_dev, x_hbm, dy_hbm, wq_hbm, wk_hbm, wv_hbm, wo_hbm, out_v,
           x_v, dy_v, wq_v, wk_v, wv_v, wo_v, wf_v, wkv_v,
           kv_send, kvbuf, q_send, do_send, qbuf, dobuf,
           est, dpst, m_run, l_run, d_run, m_ent, p_buf, ds_buf, dqt,
           pacc, pown, m1_lf, m1_rt, fin, fin_own, dq_send, dq_rows, acc, dkv, dq_tmp, wkvt,
           ld_sem, kvs, kvr, kvps, kvrs, qs, qr, m1s, m1r, m2s, m2r, fos, dqs, dqr):
    me = lax.axis_index("cp")
    n_chip = n_dev // 2
    c = me // 2
    h = me % 2
    ho = 1 - h
    right = lax.rem(c + 1, n_chip)
    left = lax.rem(c + n_chip - 1, n_chip)
    opp = lax.rem(c + 2, n_chip)
    rows, d_model = x_v.shape
    seg = rows // 2
    blk_len = kvbuf.shape[2]
    hd = qbuf.shape[3]
    groups = qbuf.shape[1]
    scale = hd ** -0.5
    scale2 = scale * math.log2(math.e)

    def off(blk, core):
        r = core if blk == 0 else 1 - core
        return pl.multiple_of(r * seg, seg)

    def rc(src, dst, ssem, rsem, chip, core):
        return pltpu.make_async_remote_copy(src_ref=src, dst_ref=dst, send_sem=ssem, recv_sem=rsem,
                                            device_id={"cp": chip * 2 + core}, device_id_type=MESH)

    def load(i, src, dst):
        return pltpu.make_async_copy(src, dst, ld_sem.at[i])

    ld_k, ld_v, ld_x = load(0, wk_hbm, wk_v), load(1, wv_hbm, wv_v), load(2, x_hbm, x_v)
    ld_q, ld_y = load(3, wq_hbm, wq_v), load(4, dy_hbm, dy_v)
    ld_o = []
    for i, grp in enumerate((ho, h)):
        r = pl.ds(pl.multiple_of(grp * groups * hd, hd), groups * hd)
        ld_o.append(load(5 + i, wo_hbm.at[r], wo_v.at[r]))
    for cp in (ld_k, ld_v, ld_x, ld_q):
        cp.start()

    barrier = pltpu.get_barrier_semaphore()
    for chip, core in ((c, ho), (right, 0), (right, 1), (left, 0), (left, 1)):
        pl.semaphore_signal(barrier, inc=1, device_id={"cp": chip * 2 + core}, device_id_type=MESH)

    for j, (ld, w) in enumerate(((ld_k, wk_v), (ld_v, wv_v))):
        ld.wait()
        if j == 0:
            for cp in [ld_y] + ld_o:
                cp.start()
        wf_v[j] = w[...].astype(F32)
    ld_x.wait()

    def project_kv(hh):
        for j in range(2):
            wkv_v[hh, :, j * hd:(j + 1) * hd] = wf_v[j, pl.ds(hh, d_model, stride=2), :].astype(BF)
        kv_send[hh] = dot(x_v[...], wkv_v[hh]).astype(BF)

    project_kv(0)
    pl.semaphore_wait(barrier, 5)

    def kv_copies(d, hh):
        go_right = (h == d)
        chip = jnp.where(go_right, right, left)
        slot = jnp.where(go_right, LF, RT)
        return [rc(kv_send.at[hh, pl.ds(blk * seg, seg), :],
                   kvbuf.at[slot, blk, pl.ds(off(blk, h), seg), :],
                   kvs.at[d, hh, blk], kvr.at[slot, h, blk], chip, hh) for blk in range(2)]

    dirs = [kv_copies(0, 0), kv_copies(1, 0), kv_copies(0, 1), kv_copies(1, 1)]
    for cp in dirs[0] + dirs[1]:
        cp.start()
    project_kv(1)
    for blk in range(2):
        kvbuf[OWN, blk, pl.ds(off(blk, h), seg), :] = kv_send[h, blk * seg:(blk + 1) * seg, :]
    kv_sends = []
    for blk in range(2):
        kv_sends.append(rc(kv_send.at[ho, pl.ds(blk * seg, seg), :],
                           kvbuf.at[OWN, blk, pl.ds(off(blk, h), seg), :],
                           kvps.at[blk], kvr.at[OWN, h, blk], c, ho))
    for cp in kv_sends:
        cp.start()

    def project(dst, src, grp, w_is_q):
        for p in range(groups // 2):
            if w_is_q:
                a = grp * groups + 2 * p
                w = jnp.concatenate([wq_v[a], wq_v[a + 1]], axis=1)
                r = dot(src[...], w).astype(BF)
            else:
                w = wo_v[pl.ds(pl.multiple_of((grp * groups + 2 * p) * hd, hd), 2 * hd), :]
                r = dot_nt(src[...], w).astype(BF)
            for k in range(2):
                dst(2 * p + k, r[:, k * hd:(k + 1) * hd])

    def to_send(buf):
        def put(g, val):
            buf[g] = val
        return put

    def to_own(buf):
        def put(g, val):
            for t in range(2):
                buf[t, g, pl.ds(off(t, h), seg), :] = val[t * seg:(t + 1) * seg]
        return put

    def xsends(buf, dst, k):
        return [rc(buf.at[:, pl.ds(t * seg, seg), :], dst.at[t, :, pl.ds(off(t, h), seg), :],
                   qs.at[k, t], qr.at[k, t], c, ho) for t in range(2)]

    ld_q.wait()
    project(to_send(q_send), x_v, ho, True)
    q_sends = xsends(q_send, qbuf, 0)
    for cp in q_sends:
        cp.start()
    for cp in dirs[2]:
        cp.start()
    project(to_own(qbuf), x_v, h, True)
    for cp in dirs[3]:
        cp.start()
    ld_y.wait()
    ld_o[0].wait()
    project(to_send(do_send), dy_v, ho, False)
    do_sends = xsends(do_send, dobuf, 1)
    for cp in do_sends:
        cp.start()
    ld_o[1].wait()
    project(to_own(dobuf), dy_v, h, False)

    def relay(start):
        cps = []
        for core, slot, chip in ((0, LF, right), (1, RT, left)):
            for blk in range(2):
                view = kvbuf.at[slot, blk, pl.ds(off(blk, core), seg), :]
                cp = rc(view, kvbuf.at[OP, blk, pl.ds(off(blk, core), seg), :],
                        kvrs.at[core, blk], kvr.at[OP, core, blk], chip, h)
                if start:
                    rc(view, view, kvs.at[0, 0, blk], kvr.at[slot, core, blk], chip, h).wait_recv()
                    cp.start()
                cps.append(cp)
        return cps

    @pl.when(h == 0)
    def _():
        relay(True)

    def fwd(ent, t, slot, blk, diag, init):
        kv = kvbuf[slot, blk]
        k, v = kv[:, :hd], kv[:, hd:]
        for g in range(groups):
            s = dot_nt(k, qbuf[t, g]) * scale2
            dp = dot_nt(v, dobuf[t, g])
            if diag:
                key_pos = lax.broadcasted_iota(jnp.int32, s.shape, 0)
                q_pos = lax.broadcasted_iota(jnp.int32, s.shape, 1)
                s = jnp.where(key_pos > q_pos, -jnp.inf, s)
            m = jnp.max(s, axis=0, keepdims=True)
            if not init:
                m_old = m_run[t, g]
                m = jnp.maximum(m, m_old)
            e = jnp.exp2(s - m)
            l = jnp.sum(e, axis=0, keepdims=True)
            d = jnp.sum(e * dp, axis=0, keepdims=True)
            if not init:
                alpha = jnp.exp2(m_old - m)
                l = l_run[t, g] * alpha + l
                d = d_run[t, g] * alpha + d
            est[ent, g] = e
            dpst[ent, g] = dp
            m_ent[ent, g] = m
            m_run[t, g] = m
            l_run[t, g] = l
            d_run[t, g] = d

    def wait_kv(slot, core, blk):
        view = kvbuf.at[slot, blk, pl.ds(off(blk, core), seg), :]
        rc(view, view, kvs.at[0, 0, 0], kvr.at[slot, core, blk], left, h).wait_recv()

    for k, dst in enumerate((qbuf, dobuf)):
        for t in range(2):
            view = dst.at[t, :, pl.ds(off(t, ho), seg), :]
            rc(view, view, qs.at[k, t], qr.at[k, t], c, ho).wait_recv()
    for blk in range(2):
        wait_kv(OWN, ho, blk)
    m_run[0] = jnp.full(m_run.shape[1:], -jnp.inf, F32)
    l_run[0] = jnp.zeros(l_run.shape[1:], F32)
    d_run[0] = jnp.zeros(d_run.shape[1:], F32)
    fwd(1, 1, OWN, 1, True, True)
    fwd(2, 1, OWN, 0, False, False)
    @pl.when(h == 1)
    def _():
        fwd(0, 0, OWN, 0, True, False)

    @pl.when(h == 1)
    def _():
        relay(True)

    def owner_of(slot):
        return jnp.where(slot == LF, left, jnp.where(slot == RT, right, opp))

    def fwd_body(i, carry):
        slot = i + 1

        @pl.when(i == 0)
        def _():
            for blk in range(2):
                wait_kv(LF, 1, blk)

        @pl.when(i == 1)
        def _():
            for blk in range(2):
                wait_kv(RT, 0, blk)

        @pl.when(i == 2)
        def _():
            for core in range(2):
                for blk in range(2):
                    wait_kv(OP, core, blk)

        later = (owner_of(slot) > c).astype(jnp.int32)
        fwd(3 + 2 * i, 1, slot, 0, False, False)
        fwd(4 + 2 * i, later, slot, later, False, False)
        return carry

    lax.fori_loop(0, 3, fwd_body, 0)

    def finish(t):
        for g in range(groups):
            l = l_run[t, g]
            d_run[t, g] = d_run[t, g] / l
            m_run[t, g] = m_run[t, g] + jnp.log2(l)

    finish(1)

    dqt[...] = jnp.zeros_like(dqt)

    def bwd(ent, t, slot, blk):
        for g in range(groups):
            w = jnp.exp2(m_ent[ent, g] - m_run[t, g])
            p = (est[ent, g] * w).astype(BF)
            p_buf[:, g * blk_len:(g + 1) * blk_len] = p
            ds_buf[:, g * blk_len:(g + 1) * blk_len] = (
                p.astype(F32) * (dpst[ent, g] - d_run[t, g])).astype(BF)
        dk = dot(ds_buf[...], qbuf[t].reshape(groups * blk_len, hd))
        dv = dot(p_buf[...], dobuf[t].reshape(groups * blk_len, hd))
        return dk, dv

    def bwd_q(t, slot, blk):
        dqt[t] += dot(kvbuf[slot, blk][:, :hd].T, ds_buf[...])

    def put(ref, pair):
        ref[:, :hd] = pair[0]
        ref[:, hd:] = pair[1]

    def add(ref, pair):
        ref[:, :hd] += pair[0]
        ref[:, hd:] += pair[1]

    def half(ref, blk, k):
        return ref.at[blk, pl.ds(k * seg, seg), :]

    def con(blk, o, s):
        return jnp.logical_or(blk == 0, o > s)

    def via_left(s):
        return s != 0

    def meets(slot, blk, k, o, s):
        if blk == 0 or k == 1:
            here = (k == 0) == (slot == RT)
        else:
            here = via_left(s) if slot == LF else jnp.logical_not(via_left(s))
        return jnp.logical_and(con(blk, o, s), here)

    def m2copy(slot, blk, k):
        chip = right if slot == RT else left
        side = 0 if slot == RT else 1
        core = k if blk == 0 else 1 - k
        return rc(half(pacc.at[slot - 1], blk, k), fin.at[side, h, blk], m2s.at[side, blk, k],
                  m2r.at[side, h, blk], chip, core)

    def m1(blk, k, d):
        j = 2 if (k == 0 and d == 1) else blk
        return rc(half(pacc.at[OP - 1], blk, k), (m1_lf, m1_rt)[d].at[j], m1s.at[d, j], m1r.at[d, j], (right, left)[d], h)

    def m1_each(blk, f):
        @pl.when(con(blk, opp, c))
        def _():
            f(m1(blk, 1, 1))
            if blk == 0:
                f(m1(0, 0, 0))
            else:
                for d, ok in enumerate((jnp.logical_not(via_left(c)), via_left(c))):
                    @pl.when(ok)
                    def _():
                        f(m1(1, 0, d))

    def direct_each(slot, blk, f):
        o, s = (right, left) if slot == RT else (left, right)
        for k in range(2):
            @pl.when(jnp.logical_and(con(blk, o, c), jnp.logical_not(meets(slot, blk, k, o, s))))
            def _():
                f(m2copy(slot, blk, k))

    def merged_each(f):
        for blk in range(2):
            for slot, o, s in ((RT, right, left), (LF, left, right)):
                for k in range(2):
                    if (blk == 0 or k == 1) and (k == 0) != (slot == RT):
                        continue
                    d = 0 if slot == RT else 1
                    j = 2 if (k == 0 and d == 1) else blk

                    @pl.when(meets(slot, blk, k, o, s))
                    def _():
                        f((m1_lf, m1_rt)[d].at[j], m1r.at[d, j], slot, blk, k)

    first_chip = jnp.logical_not(functools.reduce(jnp.logical_or, [c > x for x in (left, right, opp)]))

    def low_block():
        @pl.when(h == 0)
        def _():
            fwd(0, 0, OWN, 0, True, False)
        finish(0)

    def bwd_body(i, carry):
        for j in range(2):
            near = (LF, RT)[j]
            slot = jnp.where(i == 0, OP, near)
            second = (i == 2) if j == 0 else (i != 1)
            later = owner_of(slot) > c
            t = jnp.where(second, later.astype(jnp.int32), 1)
            blk = jnp.where(second, later.astype(jnp.int32), 0)
            fresh = jnp.logical_or(jnp.logical_not(second), later)
            ready = jnp.where(second, True, later)
            pair = bwd(1 + 2 * slot + second.astype(jnp.int32), t, slot, blk)

            @pl.when(fresh)
            def _():
                put(pacc.at[slot - 1, blk], pair)

            @pl.when(jnp.logical_not(fresh))
            def _():
                add(pacc.at[slot - 1, 0], pair)
                pacc[slot - 1, 1] = jnp.zeros(pacc.shape[2:], F32)

            for bb in range(2):
                @pl.when(jnp.logical_and(ready, blk == bb))
                def _():
                    @pl.when(i == 0)
                    def _():
                        m1_each(bb, lambda cp: cp.start())

                    @pl.when(i != 0)
                    def _():
                        direct_each(near, bb, lambda cp: cp.start())

            bwd_q(t, slot, blk)

            if j == 0:
                @pl.when(jnp.logical_and(i == 0, jnp.logical_not(first_chip)))
                def _():
                    low_block()
        return carry

    lax.fori_loop(0, 3, bwd_body, 0)

    def merge(buf, sem, slot, blk, k):
        rc(buf, buf, m1s.at[0, 0], sem, left, h).wait_recv()
        pacc[slot - 1, blk, k * seg:(k + 1) * seg, :] += buf[...]
        m2copy(slot, blk, k).start()

    if MERGE_EARLY:
        merged_each(merge)

    @pl.when(first_chip)
    def _():
        low_block()

    put(pown.at[0], bwd(0, 0, OWN, 0))
    bwd_q(0, OWN, 0)
    put(pown.at[1], bwd(1, 1, OWN, 1))
    bwd_q(1, OWN, 1)
    add(pown.at[0], bwd(2, 1, OWN, 0))
    bwd_q(1, OWN, 0)

    fo_copies = []
    for blk in range(2):
        src = pown.at[blk, pl.ds(off(blk, ho), seg), :]
        cp = rc(src, fin_own.at[blk], fos.at[0, blk], fos.at[1, blk], c, ho)
        cp.start()
        fo_copies.append(cp)

    for t in range(2):
        for g in range(groups):
            dq = (dqt[t, :, g * blk_len:(g + 1) * blk_len] * scale).astype(BF).T
            dq_tmp[g] = dq
        for g in range(groups):
            dq_send[g, t * seg:(t + 1) * seg, :] = dq_tmp[g, pl.ds(off(t, ho), seg), :]
            dq_rows[h * groups + g, t * seg:(t + 1) * seg, :] = dq_tmp[g, pl.ds(off(t, h), seg), :]
    dq_copy = rc(dq_send, dq_rows.at[pl.ds(h * groups, groups)], dqs, dqr, c, ho)
    dq_copy.start()

    if not MERGE_EARLY:
        merged_each(merge)

    view = dq_rows.at[pl.ds(ho * groups, groups)]
    rc(dq_send, view, dqs, dqr, c, ho).wait_recv()
    for p in range(groups):
        a = 2 * p
        lhs = jnp.concatenate([dq_rows[a], dq_rows[a + 1]], axis=1)
        w = jnp.concatenate([wq_v[a], wq_v[a + 1]], axis=1)
        r = dot_nt(lhs, w)
        if p == 0:
            acc[...] = r
        else:
            acc[...] += r

    for hh in range(2):
        wkvt[hh] = wkv_v[hh].T

    for blk in range(2):
        rc(fin_own.at[blk], fin_own.at[blk], fos.at[0, blk], fos.at[1, blk], c, ho).wait_recv()
        k = h if blk == 0 else 1 - h
        for side, nb in ((0, left), (1, right)):
            if blk == 0:
                way = True
            elif side == 0:
                way = jnp.logical_and(k == 0, jnp.logical_not(via_left(opp)))
            else:
                way = jnp.logical_or(k == 1, via_left(opp))
            arrives = jnp.logical_or(con(blk, c, nb), jnp.logical_and(con(blk, c, opp), way))
            for hh in range(2):
                @pl.when(arrives)
                def _():
                    dst = fin.at[side, hh, blk]
                    rc(dst, dst, m2s.at[0, 0, 0], m2r.at[side, hh, blk], left, hh).wait_recv()

                @pl.when(jnp.logical_not(arrives))
                def _():
                    fin[side, hh, blk] = jnp.zeros(fin.shape[3:], F32)
    for blk in range(2):
        r = pl.ds(blk * seg, seg)
        for hh, loc in ((h, pown[blk, pl.ds(off(blk, h), seg), :]), (ho, fin_own[blk])):
            tot = fin[0, hh, blk] + fin[1, hh, blk] + loc
            dkv[hh, r, :hd] = (tot[:, :hd] * scale).astype(BF)
            dkv[hh, r, hd:] = tot[:, hd:].astype(BF)
    out_v[...] = (acc[...] + dot(dkv[0], wkvt[0]) + dot(dkv[1], wkvt[1])).astype(BF)

    for cp in kv_sends + sum(dirs, []) + q_sends + do_sends + relay(False) + fo_copies + [dq_copy]:
        cp.wait_send()
    for blk in range(2):
        m1_each(blk, lambda cp: cp.wait_send())
    for slot in (LF, RT):
        for blk in range(2):
            direct_each(slot, blk, lambda cp: cp.wait_send())
    merged_each(lambda buf, sem, slot, blk, k: m2copy(slot, blk, k).wait_send())


def solution(mesh):
    n_dev = mesh.shape["cp"]
    row_spec = P(("dp", "cp"), None)

    def device_fn(x_in, d_y, w_q, w_k, w_v, w_o):
        rows, d_model = x_in.shape
        q_heads, hd = w_q.shape[1], w_q.shape[2]
        kv_heads = w_k.shape[1]
        groups = q_heads // kv_heads
        seg = rows // 2
        blk = rows
        wq_t = jnp.transpose(w_q, (1, 0, 2))
        wk_r = w_k.reshape(d_model * kv_heads, hd)
        wv_r = w_v.reshape(d_model * kv_heads, hd)
        wo_r = w_o.reshape(q_heads * hd, d_model)
        vm = pltpu.VMEM
        dma = pltpu.SemaphoreType.DMA
        scratch = [
            vm((rows, d_model), BF), vm((rows, d_model), BF),
            vm((q_heads, d_model, hd), BF), vm((d_model * kv_heads, hd), BF), vm((d_model * kv_heads, hd), BF),
            vm((q_heads * hd, d_model), BF), vm((2, d_model * kv_heads, hd), F32), vm((kv_heads, d_model, 2 * hd), BF),
            vm((2, rows, 2 * hd), BF), vm((4, 2, blk, 2 * hd), BF),
            vm((groups, rows, hd), BF), vm((groups, rows, hd), BF),
            vm((2, groups, blk, hd), BF), vm((2, groups, blk, hd), BF),
            vm((9, groups, blk, blk), F32), vm((9, groups, blk, blk), F32),
            vm((2, groups, 1, blk), F32), vm((2, groups, 1, blk), F32), vm((2, groups, 1, blk), F32),
            vm((9, groups, 1, blk), F32),
            vm((blk, groups * blk), BF), vm((blk, groups * blk), BF), vm((2, hd, groups * blk), F32),
            vm((3, 2, blk, 2 * hd), F32), vm((2, blk, 2 * hd), F32),
            vm((2, seg, 2 * hd), F32), vm((3, seg, 2 * hd), F32),
            vm((2, 2, 2, seg, 2 * hd), F32), vm((2, seg, 2 * hd), F32),
            vm((groups, rows, hd), BF), vm((q_heads, rows, hd), BF), vm((rows, d_model), F32),
            vm((2, rows, 2 * hd), BF), vm((groups, blk, hd), BF), vm((kv_heads, 2 * hd, d_model), BF),
            dma((7,)), dma((2, 2, 2)), dma((4, 2, 2)), dma((2,)), dma((2, 2)), dma((2, 2)), dma((2, 2)),
            dma((2, 3)), dma((2, 3)), dma((2, 2, 2)), dma((2, 2, 2)), dma((2, 2)), dma, dma,
        ]
        res = pl.pallas_call(
            functools.partial(kernel, n_dev),
            out_shape=pltpu.VMEM((rows, d_model), BF),
            in_specs=[pl.BlockSpec(memory_space=pl.ANY)] * 6,
            out_specs=pl.BlockSpec(memory_space=pltpu.VMEM),
            scratch_shapes=scratch,
            compiler_params=pltpu.CompilerParams(collective_id=0, has_side_effects=True, vmem_limit_bytes=63 * 1024 * 1024),
        )(x_in, d_y, wq_t, wk_r, wv_r, wo_r)
        return res

    return jax.shard_map(device_fn, mesh=mesh, in_specs=(row_spec, row_spec, P(), P(), P(), P()), out_specs=row_spec, check_vma=False)
```

```python
import functools
import math

import jax
import jax.numpy as jnp
from jax import lax
from jax.experimental import pallas as pl
from jax.experimental.pallas import tpu as pltpu
from jax.sharding import PartitionSpec as P

MESH = pl.DeviceIdType.MESH
BF = jnp.bfloat16
F32 = jnp.float32
OWN, LF, RT, OP = 0, 1, 2, 3
MERGE_EARLY = True
NT = (((1,), (1,)), ((), ()))


def dot(a, b):
    return jnp.dot(a, b, preferred_element_type=F32)


def dot_nt(a, b):
    return lax.dot_general(a, b, NT, preferred_element_type=F32)


def kernel(n_dev, x_hbm, dy_hbm, wq_hbm, wk_hbm, wv_hbm, wo_hbm, out_v,
           x_v, dy_v, wq_v, wk_v, wv_v, wo_v, wf_v, wkv_v,
           kv_send, kvbuf, q_send, do_send, qbuf, dobuf,
           est, dpst, m_run, l_run, d_run, m_ent, p_buf, ds_buf, dqt,
           pacc, pown, m1_lf, m1_rt, fin, fin_own, dq_send, dq_rows, acc, dkv, dq_tmp, wkvt,
           ld_sem, kvs, kvr, kvps, kvrs, qs, qr, m1s, m1r, m2s, m2r, fos, dqs, dqr):
    me = lax.axis_index("cp")
    n_chip = n_dev // 2
    c = me // 2
    h = me % 2
    ho = 1 - h
    right = lax.rem(c + 1, n_chip)
    left = lax.rem(c + n_chip - 1, n_chip)
    opp = lax.rem(c + 2, n_chip)
    rows, d_model = x_v.shape
    seg = rows // 2
    blk_len = kvbuf.shape[2]
    hd = qbuf.shape[3]
    groups = qbuf.shape[1]
    scale = hd ** -0.5
    scale2 = scale * math.log2(math.e)

    def off(blk, core):
        r = core if blk == 0 else 1 - core
        return pl.multiple_of(r * seg, seg)

    def rc(src, dst, ssem, rsem, chip, core):
        return pltpu.make_async_remote_copy(src_ref=src, dst_ref=dst, send_sem=ssem, recv_sem=rsem,
                                            device_id={"cp": chip * 2 + core}, device_id_type=MESH)

    def load(i, src, dst):
        return pltpu.make_async_copy(src, dst, ld_sem.at[i])

    ld_k, ld_v, ld_x = load(0, wk_hbm, wk_v), load(1, wv_hbm, wv_v), load(2, x_hbm, x_v)
    ld_q, ld_y = load(3, wq_hbm, wq_v), load(4, dy_hbm, dy_v)
    ld_o = []
    for i, grp in enumerate((ho, h)):
        r = pl.ds(pl.multiple_of(grp * groups * hd, hd), groups * hd)
        ld_o.append(load(5 + i, wo_hbm.at[r], wo_v.at[r]))
    for cp in (ld_k, ld_v, ld_x, ld_q):
        cp.start()

    barrier = pltpu.get_barrier_semaphore()
    for chip, core in ((c, ho), (right, 0), (right, 1), (left, 0), (left, 1)):
        pl.semaphore_signal(barrier, inc=1, device_id={"cp": chip * 2 + core}, device_id_type=MESH)

    for j, (ld, w) in enumerate(((ld_k, wk_v), (ld_v, wv_v))):
        ld.wait()
        if j == 0:
            for cp in [ld_y] + ld_o:
                cp.start()
        wf_v[j] = w[...].astype(F32)
    ld_x.wait()

    def project_kv(hh):
        for j in range(2):
            wkv_v[hh, :, j * hd:(j + 1) * hd] = wf_v[j, pl.ds(hh, d_model, stride=2), :].astype(BF)
        kv_send[hh] = dot(x_v[...], wkv_v[hh]).astype(BF)

    project_kv(0)
    pl.semaphore_wait(barrier, 5)

    def kv_copies(d, hh):
        go_right = (h == d)
        chip = jnp.where(go_right, right, left)
        slot = jnp.where(go_right, LF, RT)
        return [rc(kv_send.at[hh, pl.ds(blk * seg, seg), :],
                   kvbuf.at[slot, blk, pl.ds(off(blk, h), seg), :],
                   kvs.at[d, hh, blk], kvr.at[slot, h, blk], chip, hh) for blk in range(2)]

    dirs = [kv_copies(0, 0), kv_copies(1, 0), kv_copies(0, 1), kv_copies(1, 1)]
    for cp in dirs[0] + dirs[1]:
        cp.start()
    project_kv(1)
    for blk in range(2):
        kvbuf[OWN, blk, pl.ds(off(blk, h), seg), :] = kv_send[h, blk * seg:(blk + 1) * seg, :]
    kv_sends = []
    for blk in range(2):
        kv_sends.append(rc(kv_send.at[ho, pl.ds(blk * seg, seg), :],
                           kvbuf.at[OWN, blk, pl.ds(off(blk, h), seg), :],
                           kvps.at[blk], kvr.at[OWN, h, blk], c, ho))
    for cp in kv_sends:
        cp.start()

    def project(dst, src, grp, w_is_q):
        for p in range(groups // 2):
            if w_is_q:
                a = grp * groups + 2 * p
                w = jnp.concatenate([wq_v[a], wq_v[a + 1]], axis=1)
                r = dot(src[...], w).astype(BF)
            else:
                w = wo_v[pl.ds(pl.multiple_of((grp * groups + 2 * p) * hd, hd), 2 * hd), :]
                r = dot_nt(src[...], w).astype(BF)
            for k in range(2):
                dst(2 * p + k, r[:, k * hd:(k + 1) * hd])

    def to_send(buf):
        def put(g, val):
            buf[g] = val
        return put

    def to_own(buf):
        def put(g, val):
            for t in range(2):
                buf[t, g, pl.ds(off(t, h), seg), :] = val[t * seg:(t + 1) * seg]
        return put

    def xsends(buf, dst, k):
        return [rc(buf.at[:, pl.ds(t * seg, seg), :], dst.at[t, :, pl.ds(off(t, h), seg), :],
                   qs.at[k, t], qr.at[k, t], c, ho) for t in range(2)]

    ld_q.wait()
    project(to_send(q_send), x_v, ho, True)
    q_sends = xsends(q_send, qbuf, 0)
    for cp in q_sends:
        cp.start()
    for cp in dirs[2]:
        cp.start()
    project(to_own(qbuf), x_v, h, True)
    for cp in dirs[3]:
        cp.start()
    ld_y.wait()
    ld_o[0].wait()
    project(to_send(do_send), dy_v, ho, False)
    do_sends = xsends(do_send, dobuf, 1)
    for cp in do_sends:
        cp.start()
    ld_o[1].wait()
    project(to_own(dobuf), dy_v, h, False)

    def relay(start):
        cps = []
        for core, slot, chip in ((0, LF, right), (1, RT, left)):
            for blk in range(2):
                view = kvbuf.at[slot, blk, pl.ds(off(blk, core), seg), :]
                cp = rc(view, kvbuf.at[OP, blk, pl.ds(off(blk, core), seg), :],
                        kvrs.at[core, blk], kvr.at[OP, core, blk], chip, h)
                if start:
                    rc(view, view, kvs.at[0, 0, blk], kvr.at[slot, core, blk], chip, h).wait_recv()
                    cp.start()
                cps.append(cp)
        return cps

    @pl.when(h == 0)
    def _():
        relay(True)

    def fwd(ent, t, slot, blk, diag, init):
        kv = kvbuf[slot, blk]
        k, v = kv[:, :hd], kv[:, hd:]
        for g in range(groups):
            s = dot_nt(k, qbuf[t, g]) * scale2
            dp = dot_nt(v, dobuf[t, g])
            if diag:
                key_pos = lax.broadcasted_iota(jnp.int32, s.shape, 0)
                q_pos = lax.broadcasted_iota(jnp.int32, s.shape, 1)
                s = jnp.where(key_pos > q_pos, -jnp.inf, s)
            m = jnp.max(s, axis=0, keepdims=True)
            if not init:
                m_old = m_run[t, g]
                m = jnp.maximum(m, m_old)
            e = jnp.exp2(s - m)
            l = jnp.sum(e, axis=0, keepdims=True)
            d = jnp.sum(e * dp, axis=0, keepdims=True)
            if not init:
                alpha = jnp.exp2(m_old - m)
                l = l_run[t, g] * alpha + l
                d = d_run[t, g] * alpha + d
            est[ent, g] = e
            dpst[ent, g] = dp
            m_ent[ent, g] = m
            m_run[t, g] = m
            l_run[t, g] = l
            d_run[t, g] = d

    def wait_kv(slot, core, blk):
        view = kvbuf.at[slot, blk, pl.ds(off(blk, core), seg), :]
        rc(view, view, kvs.at[0, 0, 0], kvr.at[slot, core, blk], left, h).wait_recv()

    for k, dst in enumerate((qbuf, dobuf)):
        for t in range(2):
            view = dst.at[t, :, pl.ds(off(t, ho), seg), :]
            rc(view, view, qs.at[k, t], qr.at[k, t], c, ho).wait_recv()
    for blk in range(2):
        wait_kv(OWN, ho, blk)
    m_run[0] = jnp.full(m_run.shape[1:], -jnp.inf, F32)
    l_run[0] = jnp.zeros(l_run.shape[1:], F32)
    d_run[0] = jnp.zeros(d_run.shape[1:], F32)
    fwd(1, 1, OWN, 1, True, True)
    fwd(2, 1, OWN, 0, False, False)
    @pl.when(h == 1)
    def _():
        fwd(0, 0, OWN, 0, True, False)

    @pl.when(h == 1)
    def _():
        relay(True)

    def owner_of(slot):
        return jnp.where(slot == LF, left, jnp.where(slot == RT, right, opp))

    def fwd_body(i, carry):
        slot = i + 1

        @pl.when(i == 0)
        def _():
            for blk in range(2):
                wait_kv(LF, 1, blk)

        @pl.when(i == 1)
        def _():
            for blk in range(2):
                wait_kv(RT, 0, blk)

        @pl.when(i == 2)
        def _():
            for core in range(2):
                for blk in range(2):
                    wait_kv(OP, core, blk)

        later = (owner_of(slot) > c).astype(jnp.int32)
        fwd(3 + 2 * i, 1, slot, 0, False, False)
        fwd(4 + 2 * i, later, slot, later, False, False)
        return carry

    lax.fori_loop(0, 3, fwd_body, 0)

    def finish(t):
        for g in range(groups):
            l = l_run[t, g]
            d_run[t, g] = d_run[t, g] / l
            m_run[t, g] = m_run[t, g] + jnp.log2(l)

    finish(1)

    dqt[...] = jnp.zeros_like(dqt)

    def bwd(ent, t, slot, blk):
        for g in range(groups):
            w = jnp.exp2(m_ent[ent, g] - m_run[t, g])
            p = (est[ent, g] * w).astype(BF)
            p_buf[:, g * blk_len:(g + 1) * blk_len] = p
            ds_buf[:, g * blk_len:(g + 1) * blk_len] = (
                p.astype(F32) * (dpst[ent, g] - d_run[t, g])).astype(BF)
        dk = dot(ds_buf[...], qbuf[t].reshape(groups * blk_len, hd))
        dv = dot(p_buf[...], dobuf[t].reshape(groups * blk_len, hd))
        return dk, dv

    def bwd_q(t, slot, blk):
        dqt[t] += dot(kvbuf[slot, blk][:, :hd].T, ds_buf[...])

    def put(ref, pair):
        ref[:, :hd] = pair[0]
        ref[:, hd:] = pair[1]

    def add(ref, pair):
        ref[:, :hd] += pair[0]
        ref[:, hd:] += pair[1]

    def half(ref, blk, k):
        return ref.at[blk, pl.ds(k * seg, seg), :]

    def con(blk, o, s):
        return jnp.logical_or(blk == 0, o > s)

    def via_left(s):
        return s != 0

    def meets(slot, blk, k, o, s):
        if blk == 0 or k == 1:
            here = (k == 0) == (slot == RT)
        else:
            here = via_left(s) if slot == LF else jnp.logical_not(via_left(s))
        return jnp.logical_and(con(blk, o, s), here)

    def m2copy(slot, blk, k):
        chip = right if slot == RT else left
        side = 0 if slot == RT else 1
        core = k if blk == 0 else 1 - k
        return rc(half(pacc.at[slot - 1], blk, k), fin.at[side, h, blk], m2s.at[side, blk, k],
                  m2r.at[side, h, blk], chip, core)

    def m1(blk, k, d):
        j = 2 if (k == 0 and d == 1) else blk
        return rc(half(pacc.at[OP - 1], blk, k), (m1_lf, m1_rt)[d].at[j], m1s.at[d, j], m1r.at[d, j], (right, left)[d], h)

    def m1_each(blk, f):
        @pl.when(con(blk, opp, c))
        def _():
            f(m1(blk, 1, 1))
            if blk == 0:
                f(m1(0, 0, 0))
            else:
                for d, ok in enumerate((jnp.logical_not(via_left(c)), via_left(c))):
                    @pl.when(ok)
                    def _():
                        f(m1(1, 0, d))

    def direct_each(slot, blk, f):
        o, s = (right, left) if slot == RT else (left, right)
        for k in range(2):
            @pl.when(jnp.logical_and(con(blk, o, c), jnp.logical_not(meets(slot, blk, k, o, s))))
            def _():
                f(m2copy(slot, blk, k))

    def merged_each(f):
        for blk in range(2):
            for slot, o, s in ((RT, right, left), (LF, left, right)):
                for k in range(2):
                    if (blk == 0 or k == 1) and (k == 0) != (slot == RT):
                        continue
                    d = 0 if slot == RT else 1
                    j = 2 if (k == 0 and d == 1) else blk

                    @pl.when(meets(slot, blk, k, o, s))
                    def _():
                        f((m1_lf, m1_rt)[d].at[j], m1r.at[d, j], slot, blk, k)

    first_chip = jnp.logical_not(functools.reduce(jnp.logical_or, [c > x for x in (left, right, opp)]))

    def low_block():
        @pl.when(h == 0)
        def _():
            fwd(0, 0, OWN, 0, True, False)
        finish(0)

    def bwd_body(i, carry):
        for j in range(2):
            near = (LF, RT)[j]
            slot = jnp.where(i == 0, OP, near)
            second = (i == 2) if j == 0 else (i != 1)
            later = owner_of(slot) > c
            t = jnp.where(second, later.astype(jnp.int32), 1)
            blk = jnp.where(second, later.astype(jnp.int32), 0)
            fresh = jnp.logical_or(jnp.logical_not(second), later)
            ready = jnp.where(second, True, later)
            pair = bwd(1 + 2 * slot + second.astype(jnp.int32), t, slot, blk)

            @pl.when(fresh)
            def _():
                put(pacc.at[slot - 1, blk], pair)

            @pl.when(jnp.logical_not(fresh))
            def _():
                add(pacc.at[slot - 1, 0], pair)
                pacc[slot - 1, 1] = jnp.zeros(pacc.shape[2:], F32)

            for bb in range(2):
                @pl.when(jnp.logical_and(ready, blk == bb))
                def _():
                    @pl.when(i == 0)
                    def _():
                        m1_each(bb, lambda cp: cp.start())

                    @pl.when(i != 0)
                    def _():
                        direct_each(near, bb, lambda cp: cp.start())

            bwd_q(t, slot, blk)

            if j == 0:
                @pl.when(jnp.logical_and(i == 0, jnp.logical_not(first_chip)))
                def _():
                    low_block()
        return carry

    lax.fori_loop(0, 3, bwd_body, 0)

    def merge(buf, sem, slot, blk, k):
        rc(buf, buf, m1s.at[0, 0], sem, left, h).wait_recv()
        pacc[slot - 1, blk, k * seg:(k + 1) * seg, :] += buf[...]
        m2copy(slot, blk, k).start()

    if MERGE_EARLY:
        merged_each(merge)

    @pl.when(first_chip)
    def _():
        low_block()

    put(pown.at[0], bwd(0, 0, OWN, 0))
    bwd_q(0, OWN, 0)
    put(pown.at[1], bwd(1, 1, OWN, 1))
    bwd_q(1, OWN, 1)
    add(pown.at[0], bwd(2, 1, OWN, 0))
    bwd_q(1, OWN, 0)

    fo_copies = []
    for blk in range(2):
        src = pown.at[blk, pl.ds(off(blk, ho), seg), :]
        cp = rc(src, fin_own.at[blk], fos.at[0, blk], fos.at[1, blk], c, ho)
        cp.start()
        fo_copies.append(cp)

    for t in range(2):
        for g in range(groups):
            dq = (dqt[t, :, g * blk_len:(g + 1) * blk_len] * scale).astype(BF).T
            dq_tmp[g] = dq
        for g in range(groups):
            dq_send[g, t * seg:(t + 1) * seg, :] = dq_tmp[g, pl.ds(off(t, ho), seg), :]
            dq_rows[h * groups + g, t * seg:(t + 1) * seg, :] = dq_tmp[g, pl.ds(off(t, h), seg), :]
    dq_copy = rc(dq_send, dq_rows.at[pl.ds(h * groups, groups)], dqs, dqr, c, ho)
    dq_copy.start()

    if not MERGE_EARLY:
        merged_each(merge)

    view = dq_rows.at[pl.ds(ho * groups, groups)]
    rc(dq_send, view, dqs, dqr, c, ho).wait_recv()
    for p in range(groups):
        a = 2 * p
        lhs = jnp.concatenate([dq_rows[a], dq_rows[a + 1]], axis=1)
        w = jnp.concatenate([wq_v[a], wq_v[a + 1]], axis=1)
        r = dot_nt(lhs, w)
        if p == 0:
            acc[...] = r
        else:
            acc[...] += r

    for hh in range(2):
        wkvt[hh] = wkv_v[hh].T

    for hh in range(2):
        for blk in range(2):
            k = h if blk == 0 else 1 - h
            for side, nb in ((0, left), (1, right)):
                if blk == 0:
                    way = True
                elif side == 0:
                    way = jnp.logical_and(k == 0, jnp.logical_not(via_left(opp)))
                else:
                    way = jnp.logical_or(k == 1, via_left(opp))
                arrives = jnp.logical_or(con(blk, c, nb), jnp.logical_and(con(blk, c, opp), way))

                @pl.when(arrives)
                def _():
                    dst = fin.at[side, hh, blk]
                    rc(dst, dst, m2s.at[0, 0, 0], m2r.at[side, hh, blk], left, hh).wait_recv()

                @pl.when(jnp.logical_not(arrives))
                def _():
                    fin[side, hh, blk] = jnp.zeros(fin.shape[3:], F32)

        def total(blk, loc):
            r = pl.ds(blk * seg, seg)
            tot = fin[0, hh, blk] + fin[1, hh, blk] + loc
            dkv[hh, r, :hd] = (tot[:, :hd] * scale).astype(BF)
            dkv[hh, r, hd:] = tot[:, hd:].astype(BF)

        @pl.when(h == hh)
        def _():
            for blk in range(2):
                total(blk, pown[blk, pl.ds(off(blk, h), seg), :])

        @pl.when(h != hh)
        def _():
            for blk in range(2):
                rc(fin_own.at[blk], fin_own.at[blk], fos.at[0, blk], fos.at[1, blk], c, ho).wait_recv()
                total(blk, fin_own[blk])

        if hh == 0:
            acc[...] += dot(dkv[0], wkvt[0])
        else:
            out_v[...] = (acc[...] + dot(dkv[1], wkvt[1])).astype(BF)

    for cp in kv_sends + sum(dirs, []) + q_sends + do_sends + relay(False) + fo_copies + [dq_copy]:
        cp.wait_send()
    for blk in range(2):
        m1_each(blk, lambda cp: cp.wait_send())
    for slot in (LF, RT):
        for blk in range(2):
            direct_each(slot, blk, lambda cp: cp.wait_send())
    merged_each(lambda buf, sem, slot, blk, k: m2copy(slot, blk, k).wait_send())


def solution(mesh):
    n_dev = mesh.shape["cp"]
    row_spec = P(("dp", "cp"), None)

    def device_fn(x_in, d_y, w_q, w_k, w_v, w_o):
        rows, d_model = x_in.shape
        q_heads, hd = w_q.shape[1], w_q.shape[2]
        kv_heads = w_k.shape[1]
        groups = q_heads // kv_heads
        seg = rows // 2
        blk = rows
        wq_t = jnp.transpose(w_q, (1, 0, 2))
        wk_r = w_k.reshape(d_model * kv_heads, hd)
        wv_r = w_v.reshape(d_model * kv_heads, hd)
        wo_r = w_o.reshape(q_heads * hd, d_model)
        vm = pltpu.VMEM
        dma = pltpu.SemaphoreType.DMA
        scratch = [
            vm((rows, d_model), BF), vm((rows, d_model), BF),
            vm((q_heads, d_model, hd), BF), vm((d_model * kv_heads, hd), BF), vm((d_model * kv_heads, hd), BF),
            vm((q_heads * hd, d_model), BF), vm((2, d_model * kv_heads, hd), F32), vm((kv_heads, d_model, 2 * hd), BF),
            vm((2, rows, 2 * hd), BF), vm((4, 2, blk, 2 * hd), BF),
            vm((groups, rows, hd), BF), vm((groups, rows, hd), BF),
            vm((2, groups, blk, hd), BF), vm((2, groups, blk, hd), BF),
            vm((9, groups, blk, blk), F32), vm((9, groups, blk, blk), F32),
            vm((2, groups, 1, blk), F32), vm((2, groups, 1, blk), F32), vm((2, groups, 1, blk), F32),
            vm((9, groups, 1, blk), F32),
            vm((blk, groups * blk), BF), vm((blk, groups * blk), BF), vm((2, hd, groups * blk), F32),
            vm((3, 2, blk, 2 * hd), F32), vm((2, blk, 2 * hd), F32),
            vm((2, seg, 2 * hd), F32), vm((3, seg, 2 * hd), F32),
            vm((2, 2, 2, seg, 2 * hd), F32), vm((2, seg, 2 * hd), F32),
            vm((groups, rows, hd), BF), vm((q_heads, rows, hd), BF), vm((rows, d_model), F32),
            vm((2, rows, 2 * hd), BF), vm((groups, blk, hd), BF), vm((kv_heads, 2 * hd, d_model), BF),
            dma((7,)), dma((2, 2, 2)), dma((4, 2, 2)), dma((2,)), dma((2, 2)), dma((2, 2)), dma((2, 2)),
            dma((2, 3)), dma((2, 3)), dma((2, 2, 2)), dma((2, 2, 2)), dma((2, 2)), dma, dma,
        ]
        res = pl.pallas_call(
            functools.partial(kernel, n_dev),
            out_shape=pltpu.VMEM((rows, d_model), BF),
            in_specs=[pl.BlockSpec(memory_space=pl.ANY)] * 6,
            out_specs=pl.BlockSpec(memory_space=pltpu.VMEM),
            scratch_shapes=scratch,
            compiler_params=pltpu.CompilerParams(collective_id=0, has_side_effects=True, vmem_limit_bytes=63 * 1024 * 1024),
        )(x_in, d_y, wq_t, wk_r, wv_r, wo_r)
        return res

    return jax.shard_map(device_fn, mesh=mesh, in_specs=(row_spec, row_spec, P(), P(), P(), P()), out_specs=row_spec, check_vma=False)
```

```python
import functools
import math

import jax
import jax.numpy as jnp
from jax import lax
from jax.experimental import pallas as pl
from jax.experimental.pallas import tpu as pltpu
from jax.sharding import PartitionSpec as P

MESH = pl.DeviceIdType.MESH
BF = jnp.bfloat16
F32 = jnp.float32
OWN, LF, RT, OP = 0, 1, 2, 3
MERGE_EARLY = True
NT = (((1,), (1,)), ((), ()))


def dot(a, b):
    return jnp.dot(a, b, preferred_element_type=F32)


def dot_nt(a, b):
    return lax.dot_general(a, b, NT, preferred_element_type=F32)


def kernel(n_dev, x_hbm, dy_hbm, wq_hbm, wk_hbm, wv_hbm, wo_hbm, out_v,
           x_v, dy_v, wq_v, wk_v, wv_v, wo_v, wf_v, wkv_v,
           kv_send, kvbuf, q_send, do_send, qbuf, dobuf,
           est, dpst, m_run, l_run, d_run, m_ent, p_buf, ds_buf, dqt,
           pacc, pown, m1_lf, m1_rt, fin, fin_own, dq_send, dq_rows, acc, dkv, dq_tmp, wkvt,
           ld_sem, kvs, kvr, kvps, kvrs, qs, qr, m1s, m1r, m2s, m2r, fos, dqs, dqr):
    me = lax.axis_index("cp")
    n_chip = n_dev // 2
    c = me // 2
    h = me % 2
    ho = 1 - h
    right = lax.rem(c + 1, n_chip)
    left = lax.rem(c + n_chip - 1, n_chip)
    opp = lax.rem(c + 2, n_chip)
    rows, d_model = x_v.shape
    seg = rows // 2
    blk_len = kvbuf.shape[2]
    hd = qbuf.shape[3]
    groups = qbuf.shape[1]
    scale = hd ** -0.5
    scale2 = scale * math.log2(math.e)

    def off(blk, core):
        r = core if blk == 0 else 1 - core
        return pl.multiple_of(r * seg, seg)

    def rc(src, dst, ssem, rsem, chip, core):
        return pltpu.make_async_remote_copy(src_ref=src, dst_ref=dst, send_sem=ssem, recv_sem=rsem,
                                            device_id={"cp": chip * 2 + core}, device_id_type=MESH)

    def load(i, src, dst):
        return pltpu.make_async_copy(src, dst, ld_sem.at[i])

    ld_k, ld_v, ld_x = load(0, wk_hbm, wk_v), load(1, wv_hbm, wv_v), load(2, x_hbm, x_v)
    ld_q, ld_y = load(3, wq_hbm, wq_v), load(4, dy_hbm, dy_v)
    ld_o = []
    for i, grp in enumerate((ho, h)):
        r = pl.ds(pl.multiple_of(grp * groups * hd, hd), groups * hd)
        ld_o.append(load(5 + i, wo_hbm.at[r], wo_v.at[r]))
    for cp in (ld_k, ld_v, ld_x, ld_q):
        cp.start()

    barrier = pltpu.get_barrier_semaphore()
    for chip, core in ((c, ho), (right, 0), (right, 1), (left, 0), (left, 1)):
        pl.semaphore_signal(barrier, inc=1, device_id={"cp": chip * 2 + core}, device_id_type=MESH)

    for j, (ld, w) in enumerate(((ld_k, wk_v), (ld_v, wv_v))):
        ld.wait()
        if j == 0:
            for cp in [ld_y] + ld_o:
                cp.start()
        wf_v[j] = w[...].astype(F32)
    ld_x.wait()

    def project_kv(hh):
        for j in range(2):
            wkv_v[hh, :, j * hd:(j + 1) * hd] = wf_v[j, pl.ds(hh, d_model, stride=2), :].astype(BF)
        kv_send[hh] = dot(x_v[...], wkv_v[hh]).astype(BF)

    project_kv(0)
    pl.semaphore_wait(barrier, 5)

    def kv_copies(d, hh):
        go_right = (h == d)
        chip = jnp.where(go_right, right, left)
        slot = jnp.where(go_right, LF, RT)
        return [rc(kv_send.at[hh, pl.ds(blk * seg, seg), :],
                   kvbuf.at[slot, blk, pl.ds(off(blk, h), seg), :],
                   kvs.at[d, hh, blk], kvr.at[slot, h, blk], chip, hh) for blk in range(2)]

    dirs = [kv_copies(0, 0), kv_copies(1, 0), kv_copies(0, 1), kv_copies(1, 1)]

    def kv_each(d, f):
        f(dirs[d][0])
        dst = jnp.where(h == d % 2, right, left)

        @pl.when(jnp.logical_or(c > dst, jnp.logical_and(d % 2 == 0, c > opp)))
        def _():
            f(dirs[d][1])

    for d in (0, 1):
        kv_each(d, lambda cp: cp.start())
    project_kv(1)
    for blk in range(2):
        kvbuf[OWN, blk, pl.ds(off(blk, h), seg), :] = kv_send[h, blk * seg:(blk + 1) * seg, :]
    kv_sends = []
    for blk in range(2):
        kv_sends.append(rc(kv_send.at[ho, pl.ds(blk * seg, seg), :],
                           kvbuf.at[OWN, blk, pl.ds(off(blk, h), seg), :],
                           kvps.at[blk], kvr.at[OWN, h, blk], c, ho))
    for cp in kv_sends:
        cp.start()
    kv_each(2, lambda cp: cp.start())

    def project(dst, src, grp, w_is_q):
        for p in range(groups // 2):
            if w_is_q:
                a = grp * groups + 2 * p
                w = jnp.concatenate([wq_v[a], wq_v[a + 1]], axis=1)
                r = dot(src[...], w).astype(BF)
            else:
                w = wo_v[pl.ds(pl.multiple_of((grp * groups + 2 * p) * hd, hd), 2 * hd), :]
                r = dot_nt(src[...], w).astype(BF)
            for k in range(2):
                dst(2 * p + k, r[:, k * hd:(k + 1) * hd])

    def to_send(buf):
        def put(g, val):
            buf[g] = val
        return put

    def to_own(buf):
        def put(g, val):
            for t in range(2):
                buf[t, g, pl.ds(off(t, h), seg), :] = val[t * seg:(t + 1) * seg]
        return put

    def xsends(buf, dst, k):
        return [rc(buf.at[:, pl.ds(t * seg, seg), :], dst.at[t, :, pl.ds(off(t, h), seg), :],
                   qs.at[k, t], qr.at[k, t], c, ho) for t in range(2)]

    ld_q.wait()
    project(to_send(q_send), x_v, ho, True)
    q_sends = xsends(q_send, qbuf, 0)
    for cp in q_sends:
        cp.start()
    project(to_own(qbuf), x_v, h, True)
    kv_each(3, lambda cp: cp.start())
    ld_y.wait()
    ld_o[0].wait()
    project(to_send(do_send), dy_v, ho, False)
    do_sends = xsends(do_send, dobuf, 1)
    for cp in do_sends:
        cp.start()
    ld_o[1].wait()
    project(to_own(dobuf), dy_v, h, False)

    def relay_each(f):
        for core, slot, src, dst in ((0, LF, left, right), (1, RT, right, left)):
            for blk in range(2):
                view = kvbuf.at[slot, blk, pl.ds(off(blk, core), seg), :]
                cp = rc(view, kvbuf.at[OP, blk, pl.ds(off(blk, core), seg), :],
                        kvrs.at[core, blk], kvr.at[OP, core, blk], dst, h)
                wt = rc(view, view, kvs.at[0, 0, blk], kvr.at[slot, core, blk], dst, h)
                goes = jnp.logical_or(blk == 0, src > dst)
                f(cp, wt, jnp.logical_or(goes, src > c), goes)

    def relay_start(cp, wt, came, goes):
        pl.when(came)(lambda: wt.wait_recv())
        pl.when(goes)(lambda: cp.start())

    @pl.when(h == 0)
    def _():
        relay_each(relay_start)

    def fwd(ent, t, slot, blk, diag, init):
        kv = kvbuf[slot, blk]
        k, v = kv[:, :hd], kv[:, hd:]
        for g in range(groups):
            s = dot_nt(k, qbuf[t, g]) * scale2
            dp = dot_nt(v, dobuf[t, g])
            if diag:
                key_pos = lax.broadcasted_iota(jnp.int32, s.shape, 0)
                q_pos = lax.broadcasted_iota(jnp.int32, s.shape, 1)
                s = jnp.where(key_pos > q_pos, -jnp.inf, s)
            m = jnp.max(s, axis=0, keepdims=True)
            if not init:
                m_old = m_run[t, g]
                m = jnp.maximum(m, m_old)
            e = jnp.exp2(s - m)
            l = jnp.sum(e, axis=0, keepdims=True)
            d = jnp.sum(e * dp, axis=0, keepdims=True)
            if not init:
                alpha = jnp.exp2(m_old - m)
                l = l_run[t, g] * alpha + l
                d = d_run[t, g] * alpha + d
            est[ent, g] = e
            dpst[ent, g] = dp
            m_ent[ent, g] = m
            m_run[t, g] = m
            l_run[t, g] = l
            d_run[t, g] = d

    def wait_kv(slot, core, blk):
        view = kvbuf.at[slot, blk, pl.ds(off(blk, core), seg), :]
        rc(view, view, kvs.at[0, 0, 0], kvr.at[slot, core, blk], left, h).wait_recv()

    for k, dst in enumerate((qbuf, dobuf)):
        for t in range(2):
            view = dst.at[t, :, pl.ds(off(t, ho), seg), :]
            rc(view, view, qs.at[k, t], qr.at[k, t], c, ho).wait_recv()
    for blk in range(2):
        wait_kv(OWN, ho, blk)
    m_run[0] = jnp.full(m_run.shape[1:], -jnp.inf, F32)
    l_run[0] = jnp.zeros(l_run.shape[1:], F32)
    d_run[0] = jnp.zeros(d_run.shape[1:], F32)
    fwd(1, 1, OWN, 1, True, True)
    fwd(2, 1, OWN, 0, False, False)
    @pl.when(h == 1)
    def _():
        fwd(0, 0, OWN, 0, True, False)

    @pl.when(h == 1)
    def _():
        relay_each(relay_start)

    def owner_of(slot):
        return jnp.where(slot == LF, left, jnp.where(slot == RT, right, opp))

    def fwd_body(i, carry):
        slot = i + 1

        for n, waits in enumerate((((LF, 1),), ((RT, 0),), ((OP, 0), (OP, 1)))):
            @pl.when(i == n)
            def _():
                for sl, core in waits:
                    wait_kv(sl, core, 0)

                    @pl.when((left, right, opp)[n] > c)
                    def _():
                        wait_kv(sl, core, 1)

        later = (owner_of(slot) > c).astype(jnp.int32)
        fwd(3 + 2 * i, 1, slot, 0, False, False)
        fwd(4 + 2 * i, later, slot, later, False, False)
        return carry

    lax.fori_loop(0, 3, fwd_body, 0)

    def finish(t):
        for g in range(groups):
            l = l_run[t, g]
            d_run[t, g] = d_run[t, g] / l
            m_run[t, g] = m_run[t, g] + jnp.log2(l)

    finish(1)

    dqt[...] = jnp.zeros_like(dqt)

    def bwd(ent, t, slot, blk):
        for g in range(groups):
            w = jnp.exp2(m_ent[ent, g] - m_run[t, g])
            p = (est[ent, g] * w).astype(BF)
            p_buf[:, g * blk_len:(g + 1) * blk_len] = p
            ds_buf[:, g * blk_len:(g + 1) * blk_len] = (
                p.astype(F32) * (dpst[ent, g] - d_run[t, g])).astype(BF)
        dk = dot(ds_buf[...], qbuf[t].reshape(groups * blk_len, hd))
        dv = dot(p_buf[...], dobuf[t].reshape(groups * blk_len, hd))
        return dk, dv

    def bwd_q(t, slot, blk):
        dqt[t] += dot(kvbuf[slot, blk][:, :hd].T, ds_buf[...])

    def put(ref, pair):
        ref[:, :hd] = pair[0]
        ref[:, hd:] = pair[1]

    def add(ref, pair):
        ref[:, :hd] += pair[0]
        ref[:, hd:] += pair[1]

    def half(ref, blk, k):
        return ref.at[blk, pl.ds(k * seg, seg), :]

    def con(blk, o, s):
        return jnp.logical_or(blk == 0, o > s)

    def via_left(s):
        return s != 0

    def meets(slot, blk, k, o, s):
        if blk == 0 or k == 1:
            here = (k == 0) == (slot == RT)
        else:
            here = via_left(s) if slot == LF else jnp.logical_not(via_left(s))
        return jnp.logical_and(con(blk, o, s), here)

    def m2copy(slot, blk, k):
        chip = right if slot == RT else left
        side = 0 if slot == RT else 1
        core = k if blk == 0 else 1 - k
        return rc(half(pacc.at[slot - 1], blk, k), fin.at[side, h, blk], m2s.at[side, blk, k],
                  m2r.at[side, h, blk], chip, core)

    def m1(blk, k, d):
        j = 2 if (k == 0 and d == 1) else blk
        return rc(half(pacc.at[OP - 1], blk, k), (m1_lf, m1_rt)[d].at[j], m1s.at[d, j], m1r.at[d, j], (right, left)[d], h)

    def m1_each(blk, f):
        @pl.when(con(blk, opp, c))
        def _():
            f(m1(blk, 1, 1))
            if blk == 0:
                f(m1(0, 0, 0))
            else:
                for d, ok in enumerate((jnp.logical_not(via_left(c)), via_left(c))):
                    @pl.when(ok)
                    def _():
                        f(m1(1, 0, d))

    def direct_each(slot, blk, f):
        o, s = (right, left) if slot == RT else (left, right)
        for k in range(2):
            @pl.when(jnp.logical_and(con(blk, o, c), jnp.logical_not(meets(slot, blk, k, o, s))))
            def _():
                f(m2copy(slot, blk, k))

    def merged_each(f):
        for blk in range(2):
            for slot, o, s in ((RT, right, left), (LF, left, right)):
                for k in range(2):
                    if (blk == 0 or k == 1) and (k == 0) != (slot == RT):
                        continue
                    d = 0 if slot == RT else 1
                    j = 2 if (k == 0 and d == 1) else blk

                    @pl.when(meets(slot, blk, k, o, s))
                    def _():
                        f((m1_lf, m1_rt)[d].at[j], m1r.at[d, j], slot, blk, k)

    first_chip = jnp.logical_not(functools.reduce(jnp.logical_or, [c > x for x in (left, right, opp)]))

    def low_block():
        @pl.when(h == 0)
        def _():
            fwd(0, 0, OWN, 0, True, False)
        finish(0)

    def bwd_body(i, carry):
        for j in range(2):
            near = (LF, RT)[j]
            slot = jnp.where(i == 0, OP, near)
            second = (i == 2) if j == 0 else (i != 1)
            later = owner_of(slot) > c
            t = jnp.where(second, later.astype(jnp.int32), 1)
            blk = jnp.where(second, later.astype(jnp.int32), 0)
            fresh = jnp.logical_or(jnp.logical_not(second), later)
            ready = jnp.where(second, True, later)
            pair = bwd(1 + 2 * slot + second.astype(jnp.int32), t, slot, blk)

            @pl.when(fresh)
            def _():
                put(pacc.at[slot - 1, blk], pair)

            @pl.when(jnp.logical_not(fresh))
            def _():
                add(pacc.at[slot - 1, 0], pair)
                pacc[slot - 1, 1] = jnp.zeros(pacc.shape[2:], F32)

            for bb in range(2):
                @pl.when(jnp.logical_and(ready, blk == bb))
                def _():
                    @pl.when(i == 0)
                    def _():
                        m1_each(bb, lambda cp: cp.start())

                    @pl.when(i != 0)
                    def _():
                        direct_each(near, bb, lambda cp: cp.start())

            bwd_q(t, slot, blk)

            if j == 0:
                @pl.when(jnp.logical_and(i == 0, jnp.logical_not(first_chip)))
                def _():
                    low_block()
        return carry

    lax.fori_loop(0, 3, bwd_body, 0)

    def merge(buf, sem, slot, blk, k):
        rc(buf, buf, m1s.at[0, 0], sem, left, h).wait_recv()
        pacc[slot - 1, blk, k * seg:(k + 1) * seg, :] += buf[...]
        m2copy(slot, blk, k).start()

    if MERGE_EARLY:
        merged_each(merge)

    @pl.when(first_chip)
    def _():
        low_block()

    put(pown.at[0], bwd(0, 0, OWN, 0))
    bwd_q(0, OWN, 0)
    put(pown.at[1], bwd(1, 1, OWN, 1))
    bwd_q(1, OWN, 1)
    add(pown.at[0], bwd(2, 1, OWN, 0))
    bwd_q(1, OWN, 0)

    fo_copies = []
    for blk in range(2):
        src = pown.at[blk, pl.ds(off(blk, ho), seg), :]
        cp = rc(src, fin_own.at[blk], fos.at[0, blk], fos.at[1, blk], c, ho)
        cp.start()
        fo_copies.append(cp)

    for t in range(2):
        for g in range(groups):
            dq = (dqt[t, :, g * blk_len:(g + 1) * blk_len] * scale).astype(BF).T
            dq_tmp[g] = dq
        for g in range(groups):
            dq_send[g, t * seg:(t + 1) * seg, :] = dq_tmp[g, pl.ds(off(t, ho), seg), :]
            dq_rows[h * groups + g, t * seg:(t + 1) * seg, :] = dq_tmp[g, pl.ds(off(t, h), seg), :]
    dq_copy = rc(dq_send, dq_rows.at[pl.ds(h * groups, groups)], dqs, dqr, c, ho)
    dq_copy.start()

    if not MERGE_EARLY:
        merged_each(merge)

    view = dq_rows.at[pl.ds(ho * groups, groups)]
    rc(dq_send, view, dqs, dqr, c, ho).wait_recv()
    for p in range(groups):
        a = 2 * p
        lhs = jnp.concatenate([dq_rows[a], dq_rows[a + 1]], axis=1)
        w = jnp.concatenate([wq_v[a], wq_v[a + 1]], axis=1)
        r = dot_nt(lhs, w)
        if p == 0:
            acc[...] = r
        else:
            acc[...] += r

    for hh in range(2):
        wkvt[hh] = wkv_v[hh].T

    for hh in range(2):
        for blk in range(2):
            k = h if blk == 0 else 1 - h
            for side, nb in ((0, left), (1, right)):
                if blk == 0:
                    way = True
                elif side == 0:
                    way = jnp.logical_and(k == 0, jnp.logical_not(via_left(opp)))
                else:
                    way = jnp.logical_or(k == 1, via_left(opp))
                arrives = jnp.logical_or(con(blk, c, nb), jnp.logical_and(con(blk, c, opp), way))

                @pl.when(arrives)
                def _():
                    dst = fin.at[side, hh, blk]
                    rc(dst, dst, m2s.at[0, 0, 0], m2r.at[side, hh, blk], left, hh).wait_recv()

                @pl.when(jnp.logical_not(arrives))
                def _():
                    fin[side, hh, blk] = jnp.zeros(fin.shape[3:], F32)

        def total(blk, loc):
            r = pl.ds(blk * seg, seg)
            tot = fin[0, hh, blk] + fin[1, hh, blk] + loc
            dkv[hh, r, :hd] = (tot[:, :hd] * scale).astype(BF)
            dkv[hh, r, hd:] = tot[:, hd:].astype(BF)

        @pl.when(h == hh)
        def _():
            for blk in range(2):
                total(blk, pown[blk, pl.ds(off(blk, h), seg), :])

        @pl.when(h != hh)
        def _():
            for blk in range(2):
                rc(fin_own.at[blk], fin_own.at[blk], fos.at[0, blk], fos.at[1, blk], c, ho).wait_recv()
                total(blk, fin_own[blk])

        if hh == 0:
            acc[...] += dot(dkv[0], wkvt[0])
        else:
            out_v[...] = (acc[...] + dot(dkv[1], wkvt[1])).astype(BF)

    for cp in kv_sends + q_sends + do_sends + fo_copies + [dq_copy]:
        cp.wait_send()
    for d in range(4):
        kv_each(d, lambda cp: cp.wait_send())
    relay_each(lambda cp, wt, came, goes: pl.when(goes)(lambda: cp.wait_send()))
    for blk in range(2):
        m1_each(blk, lambda cp: cp.wait_send())
    for slot in (LF, RT):
        for blk in range(2):
            direct_each(slot, blk, lambda cp: cp.wait_send())
    merged_each(lambda buf, sem, slot, blk, k: m2copy(slot, blk, k).wait_send())


def solution(mesh):
    n_dev = mesh.shape["cp"]
    row_spec = P(("dp", "cp"), None)

    def device_fn(x_in, d_y, w_q, w_k, w_v, w_o):
        rows, d_model = x_in.shape
        q_heads, hd = w_q.shape[1], w_q.shape[2]
        kv_heads = w_k.shape[1]
        groups = q_heads // kv_heads
        seg = rows // 2
        blk = rows
        wq_t = jnp.transpose(w_q, (1, 0, 2))
        wk_r = w_k.reshape(d_model * kv_heads, hd)
        wv_r = w_v.reshape(d_model * kv_heads, hd)
        wo_r = w_o.reshape(q_heads * hd, d_model)
        vm = pltpu.VMEM
        dma = pltpu.SemaphoreType.DMA
        scratch = [
            vm((rows, d_model), BF), vm((rows, d_model), BF),
            vm((q_heads, d_model, hd), BF), vm((d_model * kv_heads, hd), BF), vm((d_model * kv_heads, hd), BF),
            vm((q_heads * hd, d_model), BF), vm((2, d_model * kv_heads, hd), F32), vm((kv_heads, d_model, 2 * hd), BF),
            vm((2, rows, 2 * hd), BF), vm((4, 2, blk, 2 * hd), BF),
            vm((groups, rows, hd), BF), vm((groups, rows, hd), BF),
            vm((2, groups, blk, hd), BF), vm((2, groups, blk, hd), BF),
            vm((9, groups, blk, blk), F32), vm((9, groups, blk, blk), F32),
            vm((2, groups, 1, blk), F32), vm((2, groups, 1, blk), F32), vm((2, groups, 1, blk), F32),
            vm((9, groups, 1, blk), F32),
            vm((blk, groups * blk), BF), vm((blk, groups * blk), BF), vm((2, hd, groups * blk), F32),
            vm((3, 2, blk, 2 * hd), F32), vm((2, blk, 2 * hd), F32),
            vm((2, seg, 2 * hd), F32), vm((3, seg, 2 * hd), F32),
            vm((2, 2, 2, seg, 2 * hd), F32), vm((2, seg, 2 * hd), F32),
            vm((groups, rows, hd), BF), vm((q_heads, rows, hd), BF), vm((rows, d_model), F32),
            vm((2, rows, 2 * hd), BF), vm((groups, blk, hd), BF), vm((kv_heads, 2 * hd, d_model), BF),
            dma((7,)), dma((2, 2, 2)), dma((4, 2, 2)), dma((2,)), dma((2, 2)), dma((2, 2)), dma((2, 2)),
            dma((2, 3)), dma((2, 3)), dma((2, 2, 2)), dma((2, 2, 2)), dma((2, 2)), dma, dma,
        ]
        res = pl.pallas_call(
            functools.partial(kernel, n_dev),
            out_shape=pltpu.VMEM((rows, d_model), BF),
            in_specs=[pl.BlockSpec(memory_space=pl.ANY)] * 6,
            out_specs=pl.BlockSpec(memory_space=pltpu.VMEM),
            scratch_shapes=scratch,
            compiler_params=pltpu.CompilerParams(collective_id=0, has_side_effects=True, vmem_limit_bytes=63 * 1024 * 1024),
        )(x_in, d_y, wq_t, wk_r, wv_r, wo_r)
        return res

    return jax.shard_map(device_fn, mesh=mesh, in_specs=(row_spec, row_spec, P(), P(), P(), P()), out_specs=row_spec, check_vma=False)
```
